32 devices in a mesh: rep: 4 (over x, y), dp: 8 (over z, core).
Axes of the slice: x: 2, y: 2, z: 4, core: 2. Of those that a mesh axis runs over, the one named last changes fastest.
Arguments:
- x: bfloat16 [32, 1024, 1024], P(('rep', 'dp')), parts along dimension 0
- dy: bfloat16 [32, 1024, 1024], P(('rep', 'dp')), parts along dimension 0
- wq: bfloat16 [2, 1024, 1024], P(None, 'dp')
- wk: bfloat16 [2, 1024, 256], P(None, 'dp')
- wv: bfloat16 [2, 1024, 256], P(None, 'dp')
- wo: bfloat16 [2, 1024, 1024], P(None, 'dp')
- w_gate: bfloat16 [2, 1024, 3200], P(None, 'dp')
- w_up: bfloat16 [2, 1024, 3200], P(None, 'dp')
- w_down: bfloat16 [2, 3200, 1024], P(None, 'dp')
- m_wq: float32 [2, 1024, 1024], P(None, 'dp')
- m_wk: float32 [2, 1024, 256], P(None, 'dp')
- m_wv: float32 [2, 1024, 256], P(None, 'dp')
- m_wo: float32 [2, 1024, 1024], P(None, 'dp')
- m_w_gate: float32 [2, 1024, 3200], P(None, 'dp')
- m_w_up: float32 [2, 1024, 3200], P(None, 'dp')
- m_w_down: float32 [2, 3200, 1024], P(None, 'dp')
- v_wq: float32 [2, 1024, 1024], P(None, 'dp')
- v_wk: float32 [2, 1024, 256], P(None, 'dp')
- v_wv: float32 [2, 1024, 256], P(None, 'dp')
- v_wo: float32 [2, 1024, 1024], P(None, 'dp')
- v_w_gate: float32 [2, 1024, 3200], P(None, 'dp')
- v_w_up: float32 [2, 1024, 3200], P(None, 'dp')
- v_w_down: float32 [2, 3200, 1024], P(None, 'dp')
Outputs:
- output 1: bfloat16 [8, 1024, 1024], P('rep', 'dp'), parts along dimension 0
- output 2: bfloat16 [8, 1024, 256], P('rep', 'dp'), parts along dimension 0
- output 3: bfloat16 [8, 1024, 256], P('rep', 'dp'), parts along dimension 0
- output 4: bfloat16 [8, 1024, 1024], P('rep', 'dp'), parts along dimension 0
- output 5: bfloat16 [8, 1024, 3200], P('rep', 'dp'), parts along dimension 0
- output 6: bfloat16 [8, 1024, 3200], P('rep', 'dp'), parts along dimension 0
- output 7: bfloat16 [8, 3200, 1024], P('rep', 'dp'), parts along dimension 0
- output 8: float32 [8, 1024, 1024], P('rep', 'dp'), parts along dimension 0
- output 9: float32 [8, 1024, 256], P('rep', 'dp'), parts along dimension 0
- output 10: float32 [8, 1024, 256], P('rep', 'dp'), parts along dimension 0
- output 11: float32 [8, 1024, 1024], P('rep', 'dp'), parts along dimension 0
- output 12: float32 [8, 1024, 3200], P('rep', 'dp'), parts along dimension 0
- output 13: float32 [8, 1024, 3200], P('rep', 'dp'), parts along dimension 0
- output 14: float32 [8, 3200, 1024], P('rep', 'dp'), parts along dimension 0
- output 15: float32 [8, 1024, 1024], P('rep', 'dp'), parts along dimension 0
- output 16: float32 [8, 1024, 256], P('rep', 'dp'), parts along dimension 0
- output 17: float32 [8, 1024, 256], P('rep', 'dp'), parts along dimension 0
- output 18: float32 [8, 1024, 1024], P('rep', 'dp'), parts along dimension 0
- output 19: float32 [8, 1024, 3200], P('rep', 'dp'), parts along dimension 0
- output 20: float32 [8, 1024, 3200], P('rep', 'dp'), parts along dimension 0
- output 21: float32 [8, 3200, 1024], P('rep', 'dp'), parts along dimension 0
There are 4 independent parts. The reference program is written for one: setup_inputs(seed, part) draws one part's arguments, and reference() takes and returns one part's arrays. A program takes and returns all parts, laid end to end along the dimension named above; an argument that names none is the same for every part.
All inputs are finite; a program needn't handle non-finite values.
Results may differ from the reference program's by a relative error of at most 0.024.
Values are sent between devices in bfloat16 or wider.
A program may use at most 2 GiB of HBM per device.

```python
import jax
import jax.numpy as jnp
from jax import lax

SEQUENCES = 8
TOKENS = 1024
D = 1024
HEADS = 8
KV_HEADS = 2
HEAD = 128
FF = 3200
LAYERS = 2
THETA = 10000
NAMES = ("wq", "wk", "wv", "wo", "w_gate", "w_up", "w_down")
SHAPES = {
    "wq": (LAYERS, D, HEADS * HEAD),
    "wk": (LAYERS, D, KV_HEADS * HEAD),
    "wv": (LAYERS, D, KV_HEADS * HEAD),
    "wo": (LAYERS, HEADS * HEAD, D),
    "w_gate": (LAYERS, D, FF),
    "w_up": (LAYERS, D, FF),
    "w_down": (LAYERS, FF, D),
}


def bump(key, n, height):
    away = (jnp.arange(n, dtype=jnp.int32) - jax.random.randint(key, (), 0, n, jnp.int32)) % n
    return jnp.where(away < n // 8, height, 1.0)


def together(key, own, strength):
    shared = jax.random.normal(key, own.shape[1:], jnp.float32)
    return (own + strength * shared) * lax.rsqrt(1 + strength * strength)


def setup_inputs(seed: int = 0, part: int = 0) -> dict:
    kx, kdy, ka, kb, kz, kf, kh, kl, *keys = jax.random.split(jax.random.key(seed), 8 + 3 * len(NAMES))
    kx, kdy, ka, kb = (jax.random.fold_in(k, part) for k in (kx, kdy, ka, kb))
    kw, km, kv = (keys[i::3] for i in range(3))
    shape = (SEQUENCES, TOKENS, D)
    much_x, much_dy = jax.random.uniform(kz, (2,), jnp.float32, 0.0, 1.0)
    loud = 2.0 ** jax.random.uniform(jax.random.fold_in(kz, 1), (), jnp.float32, -1.0, 2.0)
    layers = 2.0 ** jax.random.uniform(kl, (LAYERS, 1, 1), jnp.float32, -1.0, 1.0)
    times = {"wq": 1.0, "wk": 1.0, "wv": 2.0, "wo": layers, "w_gate": 1.0, "w_up": bump(kh, FF, 4.0), "w_down": layers}
    x = together(ka, jax.random.normal(kx, shape, jnp.float32), much_x) * bump(kf, D, 4.0)
    dy = together(kb, jax.random.normal(kdy, shape, jnp.float32), much_dy)
    drawn = {"x": x.astype(jnp.bfloat16), "dy": (loud * dy * (SEQUENCES * TOKENS) ** -0.5).astype(jnp.bfloat16)}
    for key, name in zip(kw, NAMES, strict=True):
        drawn[name] = (jax.random.normal(key, SHAPES[name], jnp.float32) * SHAPES[name][1] ** -0.5 * times[name]).astype(jnp.bfloat16)
    for key, name in zip(km, NAMES, strict=True):
        drawn[f"m_{name}"] = 0.1 * jax.random.normal(key, SHAPES[name], jnp.float32)
    for key, name in zip(kv, NAMES, strict=True):
        drawn[f"v_{name}"] = jax.random.uniform(key, SHAPES[name], jnp.float32, 0.02, 0.06)
    return drawn


def matmul(a, w):
    return jnp.dot(a, w, preferred_element_type=jnp.float32).astype(jnp.bfloat16)


def normed(h):
    wide = h.astype(jnp.float32)
    scale = lax.rsqrt(jnp.mean(wide**2, -1, keepdims=True) + 1e-6)
    return (wide * scale).astype(jnp.bfloat16)


def turned(t, theta):
    half = t.shape[-1] // 2
    angle = jnp.arange(t.shape[0], dtype=jnp.float32)[:, None] * theta ** (-jnp.arange(half, dtype=jnp.float32) / half)
    cos, sin = jnp.cos(angle)[:, None], jnp.sin(angle)[:, None]
    a, b = t[..., :half].astype(jnp.float32), t[..., half:].astype(jnp.float32)
    return jnp.concatenate([a * cos - b * sin, b * cos + a * sin], -1).astype(jnp.bfloat16)


def seen_by(q, k, v):
    tokens, kv = q.shape[0], k.shape[1]
    q = q.reshape(tokens, kv, -1, q.shape[-1])
    scores = jnp.einsum("tgsd,ugd->gstu", q.astype(jnp.float32), k.astype(jnp.float32)) * q.shape[-1] ** -0.5
    place = jnp.arange(tokens)
    weights = jax.nn.softmax(jnp.where(place[:, None] >= place, scores, -jnp.inf), -1).astype(jnp.bfloat16)
    return jnp.einsum("gstu,ugd->tgsd", weights.astype(jnp.float32), v.astype(jnp.float32)).astype(jnp.bfloat16).reshape(tokens, -1)


def layer(h, w):
    a = normed(h)
    q, k = (turned(matmul(a, w[name]).reshape(h.shape[0], -1, HEAD), THETA) for name in ("wq", "wk"))
    h = h + matmul(seen_by(q, k, matmul(a, w["wv"]).reshape(h.shape[0], -1, HEAD)), w["wo"])
    b = normed(h)
    gate = jnp.dot(b, w["w_gate"], preferred_element_type=jnp.float32)
    up = jnp.dot(b, w["w_up"], preferred_element_type=jnp.float32)
    return h + matmul((jax.nn.silu(gate) * up).astype(jnp.bfloat16), w["w_down"])


def adamw(w, m, v, g):
    m = 0.9 * m + 0.1 * g
    v = 0.95 * v + 0.05 * g * g
    step = m * lax.rsqrt(v + 1e-8) + 0.1 * w
    return (w - 0.02 * step).astype(jnp.bfloat16), m, v


def clipped(gradients, sum_of_squares, count):
    factor = jnp.minimum(1.0, 0.5 * lax.rsqrt(sum_of_squares / count + 1e-30))
    return [g * factor for g in gradients]


def stack(weights, h):
    return lax.scan(lambda h, w: (layer(h, w), None), h, weights)[0]


def reference(x, dy, wq, wk, wv, wo, w_gate, w_up, w_down, m_wq, m_wk, m_wv, m_wo, m_w_gate, m_w_up, m_w_down, v_wq, v_wk, v_wv, v_wo, v_w_gate, v_w_up, v_w_down):
    weights = dict(zip(NAMES, (wq, wk, wv, wo, w_gate, w_up, w_down), strict=True))

    def take(so_far, sequence):
        h, by_y = sequence
        _, back = jax.vjp(stack, weights, h)
        by_weights, by_h = back(by_y)
        return jax.tree.map(lambda total, term: total + term.astype(jnp.float32), so_far, by_weights), by_h

    none_yet = {name: jnp.zeros(w.shape, jnp.float32) for name, w in weights.items()}
    by_weights, by_x = lax.scan(take, none_yet, (x, dy))
    gradients = [by_weights[name].astype(jnp.bfloat16).astype(jnp.float32) for name in NAMES]
    gradients = clipped(gradients, sum(jnp.sum(g * g) for g in gradients), sum(g.size for g in gradients))
    first = (m_wq, m_wk, m_wv, m_wo, m_w_gate, m_w_up, m_w_down)
    second = (v_wq, v_wk, v_wv, v_wo, v_w_gate, v_w_up, v_w_down)
    new = [adamw(weights[name].astype(jnp.float32), m, v, g) for name, m, v, g in zip(NAMES, first, second, gradients, strict=True)]
    return tuple(one[which] for which in range(3) for one in new)
```

```python
import functools

import jax
import jax.numpy as jnp
from jax import lax
from jax.experimental import pallas as pl
from jax.experimental.pallas import tpu as pltpu

NEG = -1e30
HIDDEN = 2 * NEG
LOG2E = 1.4426950408889634


def _dot(a, b):
    return jnp.dot(a, b, preferred_element_type=jnp.float32)


def _dot_turned(a, b):
    return lax.dot_general(a, b, (((1,), (1,)), ((), ())), preferred_element_type=jnp.float32)


HEAD = 128
THETA = 10000
F32, BF16 = jnp.float32, jnp.bfloat16
MESH = pl.DeviceIdType.MESH
REPS, WAYS, LINE = 4, 8, 4
BQ, BK = 512, 256
TO_Z, TO_X, TO_Y, ON, SWAP, OWN = range(6)
FAR = LINE - 1
AHEAD = 2
KINDS = ("qkv", "o", "g0", "u0", "g1", "u1", "d")
EVERY = pl.BlockSpec(memory_space=pl.ANY)
INNER = pl.BlockSpec(memory_space=pltpu.VMEM)


class Unit:
    def __init__(self, number, layer, kind, block, whole, held, first):
        self.number, self.layer, self.kind, self.block, self.whole, self.held = number, layer, kind, block, whole, held
        self.first, self.width, self.rows = first, held.shape[1], whole.shape[0] // WAYS
        self.by_columns = self.rows // REPS % 16 != 0
        self.megabytes = whole.shape[0] * self.width * 2e-6

    def own(self, place=None):
        if place is None:
            return self.block.at[self.layer, :, pl.ds(self.first, self.width)]
        if self.by_columns:
            part = self.width // REPS
            return self.block.at[self.layer, :, pl.ds(pl.multiple_of(self.first + place * part, 128), part)]
        part = self.rows // REPS
        return self.block.at[self.layer, pl.ds(pl.multiple_of(place * part, part), part), pl.ds(self.first, self.width)]

    def part(self, way, place=None):
        base = way * self.rows
        if place is None:
            return self.whole.at[pl.ds(pl.multiple_of(base, 8), self.rows), pl.ds(self.first, self.width)]
        if self.by_columns:
            part = self.width // REPS
            return self.whole.at[pl.ds(pl.multiple_of(base, 8), self.rows), pl.ds(pl.multiple_of(self.first + place * part, 128), part)]
        part = self.rows // REPS
        return self.whole.at[pl.ds(pl.multiple_of(base + place * part, part), part), pl.ds(self.first, self.width)]

    def bytes_of(self, quarters):
        if self.by_columns:
            return self.whole.at[pl.ds(0, -(-quarters // REPS) * self.rows), pl.ds(self.first, min(quarters, REPS) * self.width // REPS)]
        return self.whole.at[pl.ds(0, quarters * self.rows // REPS), pl.ds(self.first, self.width)]


def _norm(src, dst, rows=128):
    @pl.loop(0, src.shape[0] // rows)
    def _(i):
        here = pl.ds(pl.multiple_of(i * rows, rows), rows)
        wide = src[here, :].astype(F32)
        scale = lax.rsqrt(jnp.mean(wide * wide, -1, keepdims=True) + 1e-6)
        dst[here, :] = (wide * scale).astype(BF16)


def _columns(lhs, w, tiles, width, use, first=0):
    @pl.loop(first, first + tiles)
    def _(j):
        here = pl.ds(pl.multiple_of(j * width, width), width)
        use(j, here, _dot(lhs[...], w[:, here]))


def _head(n):
    return slice(n * HEAD, (n + 1) * HEAD)


def _attend_rows(iq, qkv_s, o_s, lse_s, top_s, mix_s, scale):
    heads, d = top_s.shape[0], HEAD
    group = 2 * heads // (qkv_s.shape[1] // HEAD - heads)
    e = scale * LOG2E
    rows = pl.ds(iq * BQ, BQ)
    top_s[...] = jnp.full(top_s.shape, NEG, F32)
    mix_s[...] = jnp.zeros(mix_s.shape, F32)
    ones = jnp.ones((8, BK), BF16)

    def block(j, masked):
        here = pl.ds(pl.multiple_of(j * BK, BK), BK)
        scores = [_dot_turned(qkv_s[here, _head(heads + n // group)], qkv_s[rows, _head(n)]) for n in range(heads)]
        if masked:
            gap = lax.broadcasted_iota(jnp.int32, (BK, BQ), 1) - lax.broadcasted_iota(jnp.int32, (BK, BQ), 0)
            ok = gap >= j * BK - iq * BQ
        weights, keeps = [], []
        for n, s in enumerate(scores):
            if masked:
                s = jnp.where(ok, s, HIDDEN)
            old = top_s[n : n + 1, :]
            top = jnp.maximum(old, s.max(axis=0, keepdims=True))
            top_s[n : n + 1, :] = top
            weights.append(jnp.exp2((s - top) * e).astype(BF16))
            keeps.append(jnp.exp2((old - top) * e))
        for n, (p, keep) in enumerate(zip(weights, keeps)):
            values = jnp.concatenate([qkv_s[here, _head(heads + (heads + n) // group)].T, ones], axis=0)
            mix_s[n] = mix_s[n] * keep + _dot(values, p)

    whole = iq * BQ // BK
    if whole:
        lax.fori_loop(0, whole, lambda j, _: block(j, False), None)
    lax.fori_loop(whole, whole + BQ // BK, lambda j, _: block(j, True), None)
    for n in range(heads):
        total = mix_s[n, d : d + 1, :]
        o_s[rows, _head(n)] = (mix_s[n, :d, :] * (1 / total)).T.astype(BF16)
        lse_s[n : n + 1, rows] = top_s[n : n + 1, :] * scale + jnp.log(total)


def _flip(src, dst, rows=128):
    @pl.loop(0, src.shape[0] // rows)
    def _(i):
        here = pl.ds(pl.multiple_of(i * rows, rows), rows)
        dst[:, here] = src[here, :].T


def _rows_out(lhs, rhs, out_s, dst, sems):
    high = out_s.shape[1]
    row = sems.shape[0] - 1
    steps = lhs.shape[0] // high

    def copy(i, slot):
        return pltpu.make_async_copy(out_s.at[slot], dst.at[pl.ds(pl.multiple_of(i * high, 8), high), :], sems.at[row, slot])

    @pl.loop(0, steps)
    def _(i):
        slot = lax.rem(i, 2)

        @pl.when(i >= 2)
        def _():
            copy(i - 2, slot).wait()

        out_s[slot] = _dot(lhs[pl.ds(pl.multiple_of(i * high, 8), high), :], rhs[...]).astype(BF16)
        copy(i, slot).start()

    for i in range(max(steps - 2, 0), steps):
        copy(i, i % 2).wait()


def _schedule(units, work):
    behind = dict(Z=0, P=2, F=3, S=4)
    order, here, work = [], set(), list(work)
    for u, stage in sorted(((u, s) for u in units for s in behind), key=lambda e: (e[0].number + behind[e[1]], -behind[e[1]])):
        order.append((stage, u))
        if stage == "S":
            here.add((u.layer, u.kind))
        if work and here.issuperset(work[0][0]):
            order.append(("run", work.pop(0)[1]))
    return order + [("run", w[1]) for w in work]


def _forward_pass(layers, x_ref, dy_ref, qkv_b, o_b, g_b, u_b, d_b, cos_ref, sin_ref, *refs):
    names = ["qkv", "o", "g", "u", "d", "a", "heads", "att", "lse", "hm", "b"]
    outs = [dict(zip(names, refs[n * 11 : n * 11 + 11])) for n in range(layers)]
    states, hid_t, by_wd, refs = *refs[11 * layers : 11 * layers + 3], refs[11 * layers + 3 :]
    w_qkv, w_o, w_g0, w_u0, w_g1, w_u1, w_d, h_s, a_s, qkv_s, o_s, lse_s, hm_s, hid_s, top_s, mix_s, out_s, send, recv, load, save = refs
    held = dict(zip(KINDS, (w_qkv, w_o, w_g0, w_u0, w_g1, w_u1, w_d)))
    blocks = dict(zip(KINDS, (qkv_b, o_b, g_b, u_b, g_b, u_b, d_b)))
    tokens, d = h_s.shape
    heads = lse_s.shape[0]

    rep, way = lax.axis_index("rep"), lax.axis_index("dp")
    core, z = lax.rem(way, 2), lax.div(way, 2)
    px, py = lax.div(rep, 2), lax.rem(rep, 2)
    by_x, by_y = (1 - px) * 2 + py, px * 2 + 1 - py
    other = z * 2 + 1 - core
    far = [lax.rem(z + j, LINE) * 2 + core for j in range(1, LINE)]
    third = by_y * (1 - core) + by_x * core, by_x * (1 - core) + by_y * core

    units = []
    for n in range(layers):
        for kind in KINDS:
            first = w_g0.shape[1] if kind in ("g1", "u1") else 0
            units.append(Unit(len(units), n, kind, blocks[kind], outs[n][kind.rstrip("01")], held[kind], first))

    def to(u, stage, src, dst, device):
        pltpu.make_async_remote_copy(src_ref=src, dst_ref=dst, send_sem=send.at[u.number, stage], recv_sem=recv.at[u.number, stage],
                                     device_id=device, device_id_type=MESH).start()

    def wait(u, quarters, *sems):
        for sem in sems:
            pltpu.make_async_copy(u.bytes_of(quarters), u.bytes_of(quarters), sem).wait()

    barrier = pltpu.get_barrier_semaphore()
    near = [(by_x, way), (by_y, way), (rep, other)] + [(rep, w) for w in far]
    for device in near:
        pl.semaphore_signal(barrier, inc=1, device_id=device, device_id_type=MESH)
    pl.semaphore_wait(barrier, len(near))

    def begin(u):
        for w in far:
            to(u, TO_Z, u.own(rep), u.part(way, rep), (rep, w))
        to(u, OWN, u.own(), u.part(way), (rep, other))
        pltpu.make_async_copy(u.own(), u.part(way), load.at[u.number, 1]).start()

    for u in units[:AHEAD]:
        begin(u)

    def arrived(stage, u):
        came, at_home = recv.at[u.number], load.at[u.number]
        if stage == "Z":
            wait(u, FAR, came.at[TO_Z])
            if u.number + AHEAD < len(units):
                begin(units[u.number + AHEAD])
            for w in far:
                to(u, TO_X, u.part(w, rep), u.part(w, rep), (by_x, way))
                to(u, TO_Y, u.part(w, rep), u.part(w, rep), (by_y, way))
        elif stage == "P":
            wait(u, FAR, came.at[TO_X], came.at[TO_Y])
            for w, (place, there) in zip(far, ((by_y, by_x), (by_x, by_y), third)):
                to(u, ON, u.part(w, place), u.part(w, place), (there, way))
        elif stage == "F":
            wait(u, FAR, came.at[ON])
            for w in far:
                to(u, SWAP, u.part(w), u.part(w), (rep, other))
        else:
            wait(u, FAR * REPS, came.at[SWAP])
            wait(u, REPS, came.at[OWN], at_home.at[1])
            if u.kind != "d" or u.layer < layers - 1:
                pltpu.make_async_copy(u.whole.at[:, pl.ds(u.first, u.width)], u.held, at_home.at[0]).start()

    def at_hand(n, kind):
        u = units[n * len(KINDS) + KINDS.index(kind)]
        pltpu.make_async_copy(u.whole.at[:, pl.ds(u.first, u.width)], held[kind], load.at[u.number, 0]).wait()

    saving = {}

    def keep(n, name, src, dst):
        copy = pltpu.make_async_copy(src, dst, save.at[n, names.index(name) if name in names else len(name) % 3])
        copy.start()
        saving[n, name] = copy

    def kept(n, *what):
        for name in what:
            if (n, name) in saving:
                saving.pop((n, name)).wait()

    def project(n):
        kept(n - 1, "b", "heads")
        _norm(h_s if n else x_ref, a_s)
        keep(n, "a", a_s, outs[n]["a"])
        at_hand(n, "qkv")

        def turn(j, here, acc):
            cos, sin = cos_ref[...], sin_ref[...]
            for half in range(2):
                t = acc[:, _head(half)].astype(BF16).astype(F32)
                t = (t * cos + pltpu.roll(t, HEAD // 2, 1) * sin).astype(BF16)
                qkv_s[:, pl.ds(pl.multiple_of((2 * j + half) * HEAD, HEAD), HEAD)] = t

        def value(j, here, acc):
            qkv_s[:, here] = acc.astype(BF16)

        kv = (w_qkv.shape[1] - d) // 256
        _columns(a_s, w_qkv, d // 256 + kv // 2, 256, turn)
        _columns(a_s, w_qkv, kv // 2, 256, value, d // 256 + kv // 2)
        keep(n, "heads", qkv_s, outs[n]["heads"])

    def attention_rows(n, iq):
        if iq == 0:
            kept(n - 1, "att", "lse")
        _attend_rows(iq, qkv_s, o_s, lse_s, top_s, mix_s, HEAD**-0.5)
        if (iq + 1) * BQ == tokens:
            keep(n, "att", o_s, outs[n]["att"])
            keep(n, "lse", lse_s, outs[n]["lse"])

    def attended(n):
        kept(n - 1, "hm")
        at_hand(n, "o")
        src = h_s if n else x_ref

        def add(j, here, acc):
            hm_s[:, here] = src[:, here] + acc.astype(BF16)

        _columns(o_s, w_o, d // 256, 256, add)
        keep(n, "hm", hm_s, outs[n]["hm"])
        kept(n, "a")
        _norm(hm_s, a_s)
        keep(n, "b", a_s, outs[n]["b"])

    def gated(n, part):
        at_hand(n, f"g{part}")
        at_hand(n, f"u{part}")
        offset = part * w_g0.shape[1]
        w_g, w_u = held[f"g{part}"], held[f"u{part}"]

        @pl.loop(0, w_g.shape[1] // 128)
        def _(j):
            here = pl.ds(pl.multiple_of(j * 128, 128), 128)
            both = jnp.concatenate([w_g[:, here], w_u[:, here]], 1)
            acc = _dot(a_s[...], both)
            gate, up = acc[:, :128], acc[:, 128:]
            hid_s[:, pl.ds(pl.multiple_of(offset + j * 128, 128), 128)] = (jax.nn.silu(gate) * up).astype(BF16)

    def down(n):
        kept(n - 1, "states")
        at_hand(n, "d")

        def add(j, here, acc):
            h_s[:, here] = hm_s[:, here] + acc.astype(BF16)

        _columns(hid_s, w_d, d // 256, 256, add)
        keep(n, "states", h_s, states)

    def flipped(n):
        kept(n - 1, "hid_t")
        _flip(hid_s, w_d)
        if n < layers - 1:
            keep(n, "hid_t", w_d, hid_t.at[n])

    def last_down():
        kept(layers - 2, "states")
        copy = pltpu.make_async_copy(dy_ref, h_s, save.at[layers, 0])
        copy.start()
        copy.wait()
        _rows_out(w_d, h_s, out_s, by_wd, save)

    work = []
    for n in range(layers):
        work.append(([(n, "qkv")], functools.partial(project, n)))
        for iq in range(tokens // BQ):
            work.append(([], functools.partial(attention_rows, n, iq)))
        work.append(([(n, "o")], functools.partial(attended, n)))
        work.append(([(n, "g0"), (n, "u0")], functools.partial(gated, n, 0)))
        work.append(([(n, "g1"), (n, "u1")], functools.partial(gated, n, 1)))
        if n < layers - 1:
            work.append(([(n, "d")], functools.partial(down, n)))
        work.append(([], functools.partial(flipped, n)))
    work.append(([], last_down))
    for stage, what in _schedule(units, work):
        what() if stage == "run" else arrived(stage, what)
    for n, name in list(saving):
        kept(n, name)
    for u in units:
        sent = send.at[u.number]
        wait(u, FAR, *(sent.at[stage] for stage in (TO_Z, TO_X, TO_Y, ON)))
        wait(u, FAR * REPS, sent.at[SWAP])
        wait(u, REPS, sent.at[OWN])


def turning(tokens):
    half = HEAD // 2
    angle = jnp.arange(tokens, dtype=F32)[:, None] * THETA ** (-jnp.arange(half, dtype=F32) / half)
    cos, sin = jnp.cos(angle), jnp.sin(angle)
    return jnp.concatenate([cos, cos], 1), jnp.concatenate([-sin, sin], 1)


def forward_pass(x, dy, qkv, o, g, u, d, turns):
    layers, (tokens, wide) = qkv.shape[0], x.shape
    heads, ff = wide // HEAD, d.shape[1] * WAYS
    big = lambda *shape: jax.ShapeDtypeStruct(shape, BF16)
    shapes = dict(qkv=big(wide, qkv.shape[2]), o=big(wide, wide), g=big(wide, ff), u=big(wide, ff), d=big(ff, wide), a=big(tokens, wide),
                  heads=big(tokens, qkv.shape[2]), att=big(tokens, wide), lse=jax.ShapeDtypeStruct((heads, tokens), F32),
                  hm=big(tokens, wide), b=big(tokens, wide))
    cut = (ff // 128 + 1) // 2 * 128
    vm = lambda *shape: pltpu.VMEM(shape, BF16)
    units, each = layers * len(KINDS), len(shapes)
    got = pl.pallas_call(
        functools.partial(_forward_pass, layers),
        in_specs=[INNER, EVERY] + [INNER] * 7,
        out_specs=[EVERY] * (each * layers + 3),
        out_shape=[*list(shapes.values()) * layers, big(tokens, wide), big(layers - 1, ff, tokens), big(ff, wide)],
        scratch_shapes=[vm(wide, qkv.shape[2]), vm(wide, wide), vm(wide, cut), vm(wide, cut), vm(wide, ff - cut), vm(wide, ff - cut), vm(ff, wide),
                        vm(tokens, wide), vm(tokens, wide), vm(tokens, qkv.shape[2]), vm(tokens, wide), pltpu.VMEM((heads, tokens), F32),
                        vm(tokens, wide), vm(tokens, ff), pltpu.VMEM((heads, BQ), F32), pltpu.VMEM((heads, HEAD + 8, BQ), F32),
                        vm(2, ff // 10, wide),
                        pltpu.SemaphoreType.DMA((units, 6)), pltpu.SemaphoreType.DMA((units, 6)), pltpu.SemaphoreType.DMA((units, 2)),
                        pltpu.SemaphoreType.DMA((layers + 1, each))],
        compiler_params=pltpu.CompilerParams(collective_id=0, has_side_effects=True, vmem_limit_bytes=67043328),
        cost_estimate=pl.CostEstimate(flops=120 * 10**9, bytes_accessed=2 * 10**8, transcendentals=10**7),
        name="forward_pass",
    )(x, dy, qkv, o, g, u, d, *turns)
    return [dict(zip(shapes, got[n * each : n * each + each])) for n in range(layers)], *got[each * layers :]


PAIR, FAR_ONE, FAR_TWO, LATE = range(4)
FROM_END, FROM_MID, CAME = 1, 4, 6
FETCHED = ("by", "hid_t", "b", "d", "g", "u", "hm", "att", "a", "heads", "lse", "o", "qkv", "h")
GRADS = ("d", "g", "u", "o", "qkv")


class Gradient:
    def __init__(self, number, layer, kind, whole, swapped, sums, came, out):
        self.number, self.layer, self.kind = number, layer, kind
        self.whole, self.swapped, self.sums, self.came, self.out = whole, swapped, sums, came, out
        self.rows, self.columns = out.shape

    def at(self, ref, block):
        return ref.at[pl.ds(pl.multiple_of(block * self.rows, 8), self.rows), :]


def _tiles(width, use, size=256):
    @pl.loop(0, width // size)
    def _(j):
        use(j, pl.ds(pl.multiple_of(j * size, size), size))

    if width % size:
        use(width // size, pl.ds(width // size * size, width % size))


def _columns_out(lhs, rhs, out_s, dst, sems):
    row, width = sems.shape[0] - 1, rhs.shape[1]
    steps = -(-width // 256)

    def copy(j, here, slot):
        return pltpu.make_async_copy(out_s.at[slot, :, pl.ds(0, here.size)], dst.at[:, here], sems.at[row, slot])

    def part(j, here):
        slot = lax.rem(j, 2) if not isinstance(j, int) else j % 2
        before = pl.ds(pl.multiple_of((j - 2) * 256, 256), 256)
        if isinstance(j, int):
            copy(j - 2, before, slot).wait()
        else:
            pl.when(j >= 2)(lambda: copy(j - 2, before, slot).wait())
        out_s[slot, :, : here.size] = _dot(lhs[...], rhs[:, here]).astype(BF16)
        copy(j, here, slot).start()

    _tiles(width, part)
    for j in (steps - 2, steps - 1):
        copy(j, pl.ds(j * 256, min(256, width - j * 256)), j % 2).wait()


def _norm_back(h, by_normed, by, first=False, rows=128):
    @pl.loop(0, by.shape[0] // rows)
    def _(i):
        here = pl.ds(pl.multiple_of(i * rows, rows), rows)
        wide, grad = h[here, :].astype(F32), by_normed[here, :].astype(F32)
        scale = lax.rsqrt(jnp.mean(wide * wide, -1, keepdims=True) + 1e-6)
        along = jnp.mean(wide * grad, -1, keepdims=True)
        by[here, :] = by[here, :] + (scale * grad - wide * (scale * scale * scale * along)).astype(BF16)


def _attend_rows_back(iq, qkv_s, att_s, by_att_s, lse_s, by_s, dq_s, dk_s, dv_s, cos_ref, sin_ref, scale):
    heads, d = lse_s.shape[0], HEAD
    group = 2 * heads // (qkv_s.shape[1] // HEAD - heads)
    e = scale * LOG2E
    rows = pl.ds(iq * BQ, BQ)
    dq_s[...] = jnp.zeros(dq_s.shape, F32)
    rotated = lambda t, c, s: (t * c - pltpu.roll(t, HEAD // 2, 1) * s).astype(BF16)

    for i in range(heads // group):
        mine = range(i * group, (i + 1) * group)
        lses = [lse_s[n : n + 1, rows] * LOG2E for n in mine]
        deltas = [(by_att_s[rows, _head(n)].astype(F32) * att_s[rows, _head(n)].astype(F32)).T.sum(axis=0, keepdims=True) for n in mine]

        def block(j, masked):
            here = pl.ds(pl.multiple_of(j * BK, BK), BK)
            k, v = qkv_s[here, _head(heads + i)], qkv_s[here, _head(heads + heads // group + i)]
            if masked:
                gap = lax.broadcasted_iota(jnp.int32, (BK, BQ), 1) - lax.broadcasted_iota(jnp.int32, (BK, BQ), 0)
                ok = gap >= j * BK - iq * BQ
            qs, dos = [qkv_s[rows, _head(n)] for n in mine], [by_att_s[rows, _head(n)] for n in mine]
            scores, dps = [_dot_turned(k, q) for q in qs], [_dot_turned(v, t) for t in dos]
            for x, n in enumerate(mine):
                p = jnp.exp2(scores[x] * e - lses[x])
                if masked:
                    p = jnp.where(ok, p, 0.0)
                ds = (p * (dps[x] - deltas[x])).astype(BF16)
                dv_s[i, here, :] += _dot(p.astype(BF16), dos[x])
                dk_s[i, here, :] += _dot(ds, qs[x])
                dq_s[n] += _dot(k.T, ds)

        whole = iq * BQ // BK
        if whole:
            lax.fori_loop(0, whole, lambda j, _: block(j, False), None)
        lax.fori_loop(whole, whole + BQ // BK, lambda j, _: block(j, True), None)
        for n in mine:
            dq = (dq_s[n] * scale).T.astype(BF16).astype(F32)
            by_s[rows, _head(n)] = rotated(dq, cos_ref[rows, :], sin_ref[rows, :])

    if (iq + 1) * BQ == qkv_s.shape[0]:
        for i in range(heads // group):
            dk = (dk_s[i] * scale).astype(BF16).astype(F32)
            by_s[:, _head(heads + i)] = rotated(dk, cos_ref[...], sin_ref[...])
            by_s[:, _head(heads + heads // group + i)] = dv_s[i].astype(BF16)


def _backward_pass(layers, *refs):
    names = ["qkv", "o", "g", "u", "d", "a", "heads", "att", "lse", "hm", "b"]
    saved = [dict(zip(names, refs[n * 11 : n * 11 + 11])) for n in range(layers)]
    states, hid_t, by_wd, dy, cos_ref, sin_ref = refs[11 * layers : 11 * layers + 6]
    refs = refs[11 * layers + 6 :]
    grads = []
    for n in reversed(range(layers)):
        for kind in GRADS:
            ready = kind == "d" and n == layers - 1
            take = 4 if ready else 5
            mine, refs = list(refs[:take]), refs[take:]
            grads.append(Gradient(len(grads), n, kind, *([by_wd] if ready else []), *mine))
    factor, refs = refs[0], refs[1:]
    (p1, p2, p3, bg_s, bu_s, by_s, b_s, bb_s, t_s, qkv_s, bq_s, dq_s, dk_s, dv_s, lse_s, wide_s, high_s, square_s, table_s,
     send, recv, load, store, meet) = refs
    tokens, d = by_s.shape
    heads = lse_s.shape[0]
    of = {(g.layer, g.kind): g for g in grads}

    rep, way = lax.axis_index("rep"), lax.axis_index("dp")
    core, z = lax.rem(way, 2), lax.div(way, 2)
    at_end = (z == 0) | (z == LINE - 1)
    inner = jnp.logical_not(at_end)
    on = jnp.where((z == 0) | (z == 1), 1, -1)
    chip = lambda to: (rep, to * 2 + core)
    other = (rep, z * 2 + 1 - core)
    peers = [(rep, lax.rem(way + j, WAYS)) for j in range(1, WAYS)]

    barrier = pltpu.get_barrier_semaphore()
    for device in peers:
        pl.semaphore_signal(barrier, inc=1, device_id=device, device_id_type=MESH)
    pl.semaphore_wait(barrier, len(peers))

    def remote(g, src, dst, sent, came, device):
        return pltpu.make_async_remote_copy(src_ref=src, dst_ref=dst, send_sem=send.at[g.number, sent], recv_sem=recv.at[g.number, came],
                                            device_id=device, device_id_type=MESH)

    def wait(ref, sem):
        pltpu.make_async_copy(ref, ref, sem).wait()

    def wait_block(g, *sems):
        for sem in sems:
            wait(g.at(g.came, 0), sem)

    def pair(g):
        for there in range(LINE):
            remote(g, g.at(g.whole, there * 2 + 1 - core), g.at(g.swapped, there), PAIR, PAIR, other).start()

    def added(g, jobs, after=None):
        def scoped(buf, sems):
            loads, stores, at = [], [], 0
            for parts, _ in jobs:
                mine = []
                for ref in parts:
                    mine.append(pltpu.make_async_copy(ref, buf.at[at], sems.at[at]))
                    mine[-1].start()
                    at += 1
                loads.append((mine, at - len(parts)))
            for (mine, first), (parts, to) in zip(loads, jobs):
                for c in mine:
                    c.wait()

                @pl.loop(0, g.rows // 16)
                def _(i):
                    here = pl.ds(pl.multiple_of(i * 16, 16), 16)
                    total = buf[first, here, :].astype(F32)
                    for x in range(1, len(parts)):
                        total = total + buf[first + x, here, :].astype(F32)
                    low = total.astype(BF16)
                    buf[first, here, :] = low
                    if to is g.out:
                        wide = low.astype(F32)
                        square_s[:, : g.columns] += wide * wide

                stores.append(pltpu.make_async_copy(buf.at[first], to, sems.at[first]))
                stores[-1].start()
            for x, c in enumerate(stores):
                c.wait()
                if after:
                    after(x)

        many = sum(len(parts) for parts, _ in jobs)
        pl.run_scoped(scoped, pltpu.VMEM((many, g.rows, g.columns), BF16), pltpu.SemaphoreType.DMA((many,)))

    def step_on(many):
        return jnp.clip(z + many * on, 0, LINE - 1)

    def terms(g, block):
        return [g.at(g.whole, block * 2 + core), g.at(g.swapped, block)]

    def send_sum(g, block, sent, came, to):
        remote(g, g.at(g.sums, block), g.at(g.came, came - FROM_END), sent, came, chip(to)).start()

    def summed(g):
        wait(g.swapped, recv.at[g.number, PAIR])
        far, mid, near = step_on(3), step_on(2), step_on(1)

        def send(x):
            if x < 2:
                send_sum(g, (far, mid)[x], FAR_ONE + x, FROM_END + x, near)

        pl.when(at_end)(lambda: added(g, [(terms(g, block), g.at(g.sums, block)) for block in (far, mid, near)], send))

    def late(g):
        pl.when(at_end)(lambda: send_sum(g, step_on(1), LATE, FROM_END + 2, step_on(1)))

    def sent_far(g):
        pl.when(at_end)(lambda: wait_block(g, send.at[g.number, FAR_ONE], send.at[g.number, FAR_ONE + 1]))

    def passed(g):
        far, mid = step_on(2), step_on(1)

        def jobs():
            wait_block(g, recv.at[g.number, FROM_END], recv.at[g.number, FROM_END + 1])
            added(g, [(terms(g, block) + [g.at(g.came, x)], g.at(g.sums, block)) for x, block in enumerate((far, mid))],
                  lambda x: send_sum(g, (far, mid)[x], FAR_ONE + x, FROM_MID + x, mid))

        pl.when(inner)(jobs)

    def back(g):
        end = step_on(-1)

        def jobs():
            wait_block(g, recv.at[g.number, FROM_MID])
            added(g, [(terms(g, end) + [g.at(g.came, FROM_MID - FROM_END)], g.at(g.sums, end))],
                  lambda x: send_sum(g, end, LATE, FROM_END, end))

        pl.when(inner)(jobs)

    def last(g):
        def at_inner():
            wait_block(g, recv.at[g.number, FROM_END + 2], recv.at[g.number, FROM_MID + 1])
            added(g, [(terms(g, z) + [g.at(g.came, 2), g.at(g.came, FROM_MID + 1 - FROM_END)], g.out)])

        def at_the_end():
            wait_block(g, recv.at[g.number, FROM_END])
            added(g, [(terms(g, z) + [g.at(g.came, 0)], g.out)])

        pl.when(inner)(at_inner)
        pl.when(at_end)(at_the_end)

    coming = {}

    def fetch(name, src, dst):
        copy = pltpu.make_async_copy(src, dst, load.at[FETCHED.index(name)])
        copy.start()
        coming[name] = copy

    def need(*what):
        for name in what:
            coming.pop(name).wait()

    rows_of = lambda ref, i: ref.at[pl.ds(i * d, d), :]
    att_s, hm_s, a_s = (rows_of(p3, i) for i in range(3))
    wqkv_s, wo_s = p1.at[:, pl.ds(0, qkv_s.shape[1])], p1.at[:, pl.ds(qkv_s.shape[1], d)]

    def transposed_dot(lhs, w, here):
        return _dot_turned(lhs[...], w[here, :])

    def hidden(first, many):
        def part(j, here):
            gate = _dot(b_s[...], p1[:, here])
            up = _dot(b_s[...], p2[:, here])
            by = transposed_dot(by_s, p3, here).astype(BF16).astype(F32)
            sig = jax.nn.sigmoid(gate)
            bu_s[:, here] = (by * (gate * sig)).astype(BF16)
            bg_s[:, here] = (by * up * (sig * (1 + gate * (1 - sig)))).astype(BF16)

        width = p1.shape[1]

        @pl.loop(first, min(first + many, width // 256))
        def _(j):
            part(j, pl.ds(pl.multiple_of(j * 256, 256), 256))

        if first + many > width // 256 and width % 256:
            part(width // 256, pl.ds(width // 256 * 256, width % 256))

    def project_back(w, src, dst):
        def part(j, here):
            dst[:, here] = transposed_dot(src, w, here).astype(BF16)

        _tiles(d, part)

    def by_b():
        def part(j, here):
            bb_s[:, here] = (transposed_dot(bg_s, p1, here) + transposed_dot(bu_s, p2, here)).astype(BF16)

        _tiles(d, part)

    def layer_steps(n):
        s = saved[n]
        top = n == layers - 1
        grad = lambda kind: of[n, kind]

        def start():
            if top:
                fetch("by", dy, by_s)
            else:
                fetch("hid_t", hid_t.at[n], p3)
            fetch("b", s["b"], b_s)
            if top:
                fetch("d", s["d"], p3)
            fetch("g", s["g"], p1)
            fetch("u", s["u"], p2)
            fetch("heads", s["heads"], qkv_s)
            fetch("lse", s["lse"], lse_s)
            if top:
                need("by")

        def by_down():
            need("hid_t")
            _rows_out(p3, by_s, high_s, grad("d").whole, store)
            fetch("d", s["d"], p3)

        def hidden_first():
            need("b", "d", "g", "u")
            hidden(0, 4)

        def hidden_last():
            hidden(8, 5)
            fetch("hm", s["hm"], hm_s)
            fetch("att", s["att"], att_s)
            fetch("a", s["a"], a_s)

        def by_gate():
            _flip(b_s, t_s)
            _columns_out(t_s, bg_s, wide_s, grad("g").whole, store)

        def by_up():
            _columns_out(t_s, bu_s, wide_s, grad("u").whole, store)

        def by_b_only():
            by_b()

        def by_mid():
            fetch("o", s["o"], wo_s)
            fetch("qkv", s["qkv"], wqkv_s)
            need("hm")
            _norm_back(hm_s, bb_s, by_s)

        def by_o():
            need("att")
            _flip(att_s, t_s)
            _columns_out(t_s, by_s, wide_s, grad("o").whole, store)

        def by_att():
            need("o", "heads", "lse")
            project_back(wo_s, by_s, bb_s)

        def attention(iq):
            if iq == 0:
                dk_s[...] = jnp.zeros(dk_s.shape, F32)
                dv_s[...] = jnp.zeros(dv_s.shape, F32)
            _attend_rows_back(iq, qkv_s, att_s, bb_s, lse_s, bq_s, dq_s, dk_s, dv_s, cos_ref, sin_ref, HEAD**-0.5)

        def by_qkv():
            need("a")
            _flip(a_s, t_s)
            _columns_out(t_s, bq_s, wide_s, grad("qkv").whole, store)

        def by_states():
            fetch("h", states, hm_s)
            need("qkv")
            project_back(wqkv_s, bq_s, bb_s)
            need("h")
            _norm_back(hm_s, bb_s, by_s)

        def drop():
            need("qkv")

        f = functools.partial
        do = lambda what, *kinds: [f(what, grad(kind)) for kind in kinds]
        steps = [start] if top else [start, by_down]
        steps += do(pair, "d")
        if not top:
            steps += [f(passed, of[n + 1, "qkv"])]
        early = do(summed, "d") + (do(late, "d") if top else [])
        steps += early + [hidden_first] if top else [hidden_first] + early
        steps += [f(hidden, 4, 4)] + do(passed, "d") + [hidden_last, by_gate] + do(pair, "g") + [by_up] + do(pair, "u") + do(summed, "g")
        steps += do(back, "d") + [by_b_only] + do(summed, "u") + do(passed, "g") + [by_mid, by_o] + do(pair, "o") + [by_att] + do(summed, "o")
        steps += (do(late, "g") if top else []) + [f(attention, 0)] + do(passed, "u") + do(back, "g") + [f(attention, 1), by_qkv] + do(pair, "qkv")
        steps += (do(late, "u") if top else []) + [by_states if n else drop] + do(summed, "qkv") + do(back, "u") + do(passed, "o")
        return steps

    square_s[...] = jnp.zeros(square_s.shape, F32)
    steps = []
    for n in reversed(range(layers)):
        steps += layer_steps(n)
    for step in steps:
        step()
    end, top = grads[-1], layers - 1
    waiting = [of[0, "d"], of[0, "g"], of[0, "u"], of[top, "o"], of[top, "qkv"], of[0, "o"], of[0, "qkv"]]
    sent_far(of[0, "u"])
    for g in waiting[:2]:
        late(g)
    passed(end)
    for kind in ("o", "qkv"):
        back(of[top, kind])
    for kind in ("o", "qkv"):
        back(of[0, kind])
    sent_far(end)
    for g in waiting[2:]:
        late(g)
    for g in [of[top, kind] for kind in ("d", "g", "u")] + waiting:
        last(g)

    mine = jnp.sum(square_s[...])
    table_s[way] = jnp.full(table_s.shape[1:], mine, F32)
    copies = []
    for j, device in enumerate(peers):
        copies.append(pltpu.make_async_remote_copy(src_ref=table_s.at[way], dst_ref=table_s.at[way], send_sem=meet.at[0, j],
                                                   recv_sem=meet.at[1, j], device_id=device, device_id_type=MESH))
        copies[-1].start()
    for copy in copies:
        copy.wait()
    total = table_s[0]
    for j in range(1, WAYS):
        total = total + table_s[j]
    factor[...] = total

    for g in grads:
        wait(g.swapped, send.at[g.number, PAIR])
        wait_block(g, send.at[g.number, LATE])
        if g not in (end, of[0, "u"]):
            wait_block(g, send.at[g.number, FAR_ONE], send.at[g.number, FAR_TWO])
        else:
            pl.when(inner)(lambda: wait_block(g, send.at[g.number, FAR_ONE], send.at[g.number, FAR_TWO]))


def backward_pass(saved, states, hid_t, by_wd, dy, turns):
    layers, (tokens, wide) = len(saved), dy.shape
    ff, heads = hid_t.shape[1], wide // HEAD
    three = saved[0]["qkv"].shape[1]
    big = lambda *shape: jax.ShapeDtypeStruct(shape, BF16)
    vm = lambda *shape: pltpu.VMEM(shape, BF16)
    f32 = lambda *shape: pltpu.VMEM(shape, F32)
    outs, where = [], {}
    for n in reversed(range(layers)):
        for kind in GRADS:
            rows, columns = saved[n][kind].shape
            if not (kind == "d" and n == layers - 1):
                outs.append(big(rows, columns))
            outs += [big(rows // 2, columns)] * 2 + [big(rows * (CAME - FROM_END) // WAYS, columns), big(rows // WAYS, columns)]
            where[n, kind] = len(outs) - 1
    count = len(where)
    got = pl.pallas_call(
        functools.partial(_backward_pass, layers),
        in_specs=[EVERY] * (11 * layers + 4) + [INNER] * 2,
        out_specs=[EVERY] * len(outs) + [INNER],
        out_shape=[*outs, jax.ShapeDtypeStruct((8, 128), F32)],
        scratch_shapes=[vm(wide, ff), vm(wide, ff), vm(ff, wide), vm(tokens, ff), vm(tokens, ff), *[vm(tokens, wide)] * 4, vm(tokens, three),
                        vm(tokens, three), f32(heads, HEAD, BQ), f32((three - wide) // 2 // HEAD, tokens, HEAD),
                        f32((three - wide) // 2 // HEAD, tokens, HEAD), f32(heads, tokens), vm(2, wide, 256), vm(2, ff // 10, wide),
                        f32(16, ff), f32(WAYS, 8, 128),
                        pltpu.SemaphoreType.DMA((count, LATE + 1)), pltpu.SemaphoreType.DMA((count, CAME)), pltpu.SemaphoreType.DMA((len(FETCHED),)),
                        pltpu.SemaphoreType.DMA((2, 2)), pltpu.SemaphoreType.DMA((2, WAYS - 1))],
        compiler_params=pltpu.CompilerParams(collective_id=1, has_side_effects=True, vmem_limit_bytes=67043328),
        cost_estimate=pl.CostEstimate(flops=150 * 10**9, bytes_accessed=3 * 10**8, transcendentals=10**7),
        name="backward_pass",
    )(*[t for s in saved for t in s.values()], states, hid_t, by_wd, dy, *turns)
    return [{kind: got[where[n, kind]] for kind in GRADS} for n in range(layers)], got[-1][0, 0]


from jax.sharding import PartitionSpec as P


def adamw(w, m, v, g):
    m = 0.9 * m + 0.1 * g
    v = 0.95 * v + 0.05 * g * g
    step = m * lax.rsqrt(v + 1e-8) + 0.1 * w
    return (w - 0.02 * step).astype(BF16), m, v


def solution(mesh):
    def step(x, dy, *arrays):
        weights, m, v = (arrays[i : i + 7] for i in (0, 7, 14))
        wq, wk, wv, wo, wg, wu, wd = weights
        d, kv = wq.shape[2], wk.shape[2]
        turns = turning(x.shape[1])
        saved, *rest = forward_pass(x[0], dy[0], jnp.concatenate([wq, wk, wv], 2), wo, wg, wu, wd, turns)
        parts, squares = backward_pass(saved, *rest, dy[0], turns)
        count = WAYS * sum(w.size for w in weights)
        factor = jnp.minimum(1.0, 0.5 * lax.rsqrt(squares / count + 1e-30))
        split = lambda p: (p["qkv"][:, :d], p["qkv"][:, d : d + kv], p["qkv"][:, d + kv :], p["o"], p["g"], p["u"], p["d"])
        gradients = [jnp.stack(g).astype(F32) * factor for g in zip(*(split(p) for p in parts))]
        new = [adamw(w.astype(F32), m, v, g) for w, m, v, g in zip(weights, m, v, gradients, strict=True)]
        return tuple(one[which] for which in range(3) for one in new)

    states, cut = P(("rep", "dp"), None, None), P(None, "dp", None)
    return jax.shard_map(
        step,
        mesh=mesh,
        in_specs=(states, states) + (cut,) * 21,
        out_specs=(P("rep", "dp", None),) * 21,
        check_vma=False,
    )
```

```python
import functools

import jax
import jax.numpy as jnp
from jax import lax
from jax.experimental import pallas as pl
from jax.experimental.pallas import tpu as pltpu

NEG = -1e30
HIDDEN = 2 * NEG
LOG2E = 1.4426950408889634


def _dot(a, b):
    return jnp.dot(a, b, preferred_element_type=jnp.float32)


def _dot_turned(a, b):
    return lax.dot_general(a, b, (((1,), (1,)), ((), ())), preferred_element_type=jnp.float32)


HEAD = 128
THETA = 10000
F32, BF16 = jnp.float32, jnp.bfloat16
MESH = pl.DeviceIdType.MESH
REPS, WAYS, LINE = 4, 8, 4
BQ, BK = 512, 256
TO_Z, TO_X, TO_Y, ON, SWAP, OWN = range(6)
FAR = LINE - 1
START, PACE, BEFORE = 24.0, 3.0, dict(Z=24, P=14, F=6, S=0)
AHEAD = 2
KINDS = ("qkv", "o", "g0", "u0", "g1", "u1", "g2", "u2", "d0", "d1")
PARTS = 3
WHOLE = ["qkv", "o", "g", "u", "d"]
SAVED = ["a", "heads", "att", "lse", "hm", "b", "states", "hid_t"]
GRADS = ["d", "g0", "u0", "g1", "u1", "o", "qkv"]
GRAD_ARRAYS = ["d", "g", "u", "o", "qkv"]
FETCHED = ["by", "hid_t", "b", "d", "g", "u", "hm", "att", "a", "heads", "lse", "o", "qkv", "h"]
PAIR, FAR_ONE, FAR_TWO, LATE, PAIR_LAST = range(5)
FROM_END, FROM_MID, CAME = 1, 4, 6
EVERY = pl.BlockSpec(memory_space=pl.ANY)
INNER = pl.BlockSpec(memory_space=pltpu.VMEM)


class Unit:
    def __init__(self, number, layer, kind, block, whole, held, first):
        self.number, self.layer, self.kind, self.block, self.whole, self.held = number, layer, kind, block, whole, held
        self.first, self.width, self.rows = first, held.shape[1], whole.shape[0] // WAYS
        self.by_columns = self.rows // REPS % 16 != 0

    def cut(self, ref, base, place):
        part = (self.width if self.by_columns else self.rows) // REPS
        if place is None:
            return ref.at[pl.ds(pl.multiple_of(base, 8), self.rows), pl.ds(self.first, self.width)]
        if self.by_columns:
            return ref.at[pl.ds(pl.multiple_of(base, 8), self.rows), pl.ds(pl.multiple_of(self.first + place * part, 128), part)]
        return ref.at[pl.ds(pl.multiple_of(base + place * part, part), part), pl.ds(self.first, self.width)]

    def own(self, place=None):
        return self.cut(self.block, 0, place)

    def part(self, way, place=None):
        return self.cut(self.whole, way * self.rows, place)

    def bytes_of(self, quarters):
        if self.by_columns:
            return self.whole.at[pl.ds(0, -(-quarters // REPS) * self.rows), pl.ds(self.first, min(quarters, REPS) * self.width // REPS)]
        return self.whole.at[pl.ds(0, quarters * self.rows // REPS), pl.ds(self.first, self.width)]


def _norm(src, dst, rows=128):
    @pl.loop(0, src.shape[0] // rows)
    def _(i):
        here = pl.ds(pl.multiple_of(i * rows, rows), rows)
        wide = src[here, :].astype(F32)
        scale = lax.rsqrt(jnp.mean(wide * wide, -1, keepdims=True) + 1e-6)
        dst[here, :] = (wide * scale).astype(BF16)


def _columns(lhs, w, tiles, width, use, first=0):
    @pl.loop(first, first + tiles)
    def _(j):
        here = pl.ds(pl.multiple_of(j * width, width), width)
        use(j, here, _dot(lhs[...], w[:, here]))


def _head(n):
    return slice(n * HEAD, (n + 1) * HEAD)


def _attend_rows(iq, part, qkv_s, o_s, lse_s, top_s, mix_s, scale):
    heads, d = top_s.shape[0], HEAD
    group = 2 * heads // (qkv_s.shape[1] // HEAD - heads)
    e = scale * LOG2E
    rows = pl.ds(iq * BQ, BQ)
    whole = iq * BQ // BK
    if part == 0 or not whole:
        top_s[...] = jnp.full(top_s.shape, NEG, F32)
        mix_s[...] = jnp.zeros(mix_s.shape, F32)
    ones = jnp.ones((8, BK), BF16)

    def block(j, masked):
        here = pl.ds(pl.multiple_of(j * BK, BK), BK)
        scores = [_dot_turned(qkv_s[here, _head(heads + n // group)], qkv_s[rows, _head(n)]) for n in range(heads)]
        if masked:
            gap = lax.broadcasted_iota(jnp.int32, (BK, BQ), 1) - lax.broadcasted_iota(jnp.int32, (BK, BQ), 0)
            ok = gap >= j * BK - iq * BQ
        weights, keeps = [], []
        for n, s in enumerate(scores):
            if masked:
                s = jnp.where(ok, s, HIDDEN)
            old = top_s[n : n + 1, :]
            top = jnp.maximum(old, s.max(axis=0, keepdims=True))
            top_s[n : n + 1, :] = top
            weights.append(jnp.exp2((s - top) * e).astype(BF16))
            keeps.append(jnp.exp2((old - top) * e))
        for n, (p, keep) in enumerate(zip(weights, keeps)):
            values = jnp.concatenate([qkv_s[here, _head(heads + (heads + n) // group)].T, ones], axis=0)
            mix_s[n] = mix_s[n] * keep + _dot(values, p)

    if part == 0:
        lax.fori_loop(0, whole, lambda j, _: block(j, False), None)
        return
    lax.fori_loop(whole, whole + BQ // BK, lambda j, _: block(j, True), None)
    for n in range(heads):
        total = mix_s[n, d : d + 1, :]
        o_s[rows, _head(n)] = (mix_s[n, :d, :] * (1 / total)).T.astype(BF16)
        lse_s[n : n + 1, rows] = top_s[n : n + 1, :] * scale + jnp.log(total)


def _flip(src, dst, first=0, width=None, rows=128):
    across = pl.ds(first, width or src.shape[1])

    @pl.loop(0, src.shape[0] // rows)
    def _(i):
        here = pl.ds(pl.multiple_of(i * rows, rows), rows)
        dst[across, here] = src[here, across].T


def _flip_out(src, out_s, dst, sems, first, width):
    def copy(i, slot):
        return pltpu.make_async_copy(out_s.at[slot, pl.ds(0, 128), :], dst.at[pl.ds(pl.multiple_of(i * 128, 128), 128), :], sems.at[slot])

    start, end = first // 128, (first + width) // 128

    @pl.loop(start, end)
    def _(i):
        slot = lax.rem(i, 2)

        @pl.when(i >= start + 2)
        def _():
            copy(i - 2, slot).wait()

        out_s[slot, :128, :] = src[:, pl.ds(pl.multiple_of(i * 128, 128), 128)].T
        copy(i, slot).start()

    for i in (end - 2, end - 1):
        copy(i, i % 2).wait()


def _rows_out(lhs, rhs, out_s, dst, sems, first, last):
    high = out_s.shape[1]

    def copy(i, slot):
        return pltpu.make_async_copy(out_s.at[slot], dst.at[pl.ds(pl.multiple_of(i * high, 8), high), :], sems.at[slot])

    @pl.loop(first, last)
    def _(i):
        slot = lax.rem(i, 2)

        @pl.when(i >= first + 2)
        def _():
            copy(i - 2, slot).wait()

        out_s[slot] = _dot(lhs[pl.ds(pl.multiple_of(i * high, 8), high), :], rhs[...]).astype(BF16)
        copy(i, slot).start()

    for i in (last - 2, last - 1):
        copy(i, i % 2).wait()


class Gradient:
    def __init__(self, number, layer, kind, refs, first, columns):
        self.number, self.layer, self.kind, self.first, self.columns = number, layer, kind, first, columns
        whole, self.swapped, self.sums, self.came, out = refs
        self.rows = out.shape[0]
        across = pl.ds(first, columns)
        self.whole, self.out = whole.at[:, across], out.at[:, across]
        self.across = across

    def at(self, ref, block, many=1):
        return ref.at[pl.ds(pl.multiple_of(block * self.rows, 8), many * self.rows), self.across]

    def own(self, block):
        return self.whole.at[pl.ds(pl.multiple_of(block * self.rows, 8), self.rows), :]


def _tiles(width, use, size=256):
    @pl.loop(0, width // size)
    def _(j):
        use(j, pl.ds(pl.multiple_of(j * size, size), size))

    if width % size:
        use(width // size, pl.ds(width // size * size, width % size))


def _columns_out(lhs, rhs, out_s, dst, sems):
    width = rhs.shape[1]
    steps = -(-width // 256)

    def copy(j, here, slot):
        return pltpu.make_async_copy(out_s.at[slot, :, pl.ds(0, here.size)], dst.at[:, here], sems.at[slot])

    def part(j, here):
        slot = lax.rem(j, 2) if not isinstance(j, int) else j % 2
        before = pl.ds(pl.multiple_of((j - 2) * 256, 256), 256)
        if isinstance(j, int):
            copy(j - 2, before, slot).wait()
        else:
            pl.when(j >= 2)(lambda: copy(j - 2, before, slot).wait())
        out_s[slot, :, : here.size] = _dot(lhs[...], rhs[:, here]).astype(BF16)
        copy(j, here, slot).start()

    _tiles(width, part)
    for j in (steps - 2, steps - 1):
        copy(j, pl.ds(j * 256, min(256, width - j * 256)), j % 2).wait()


def _norm_back(h, by_normed, by, first=False, rows=128):
    @pl.loop(0, by.shape[0] // rows)
    def _(i):
        here = pl.ds(pl.multiple_of(i * rows, rows), rows)
        wide, grad = h[here, :].astype(F32), by_normed[here, :].astype(F32)
        scale = lax.rsqrt(jnp.mean(wide * wide, -1, keepdims=True) + 1e-6)
        along = jnp.mean(wide * grad, -1, keepdims=True)
        by[here, :] = by[here, :] + (scale * grad - wide * (scale * scale * scale * along)).astype(BF16)


def _attend_rows_back(iq, qkv_s, att_s, by_att_s, lse_s, by_s, dq_s, dk_s, dv_s, cos_ref, sin_ref, scale):
    heads, d = lse_s.shape[0], HEAD
    group = 2 * heads // (qkv_s.shape[1] // HEAD - heads)
    e = scale * LOG2E
    rows = pl.ds(iq * BQ, BQ)
    dq_s[...] = jnp.zeros(dq_s.shape, F32)
    rotated = lambda t, c, s: (t * c - pltpu.roll(t, HEAD // 2, 1) * s).astype(BF16)

    for i in range(heads // group):
        mine = range(i * group, (i + 1) * group)
        lses = [lse_s[n : n + 1, rows] * LOG2E for n in mine]
        deltas = [(by_att_s[rows, _head(n)].astype(F32) * att_s[rows, _head(n)].astype(F32)).T.sum(axis=0, keepdims=True) for n in mine]

        def block(j, masked):
            here = pl.ds(pl.multiple_of(j * BK, BK), BK)
            k, v = qkv_s[here, _head(heads + i)], qkv_s[here, _head(heads + heads // group + i)]
            if masked:
                gap = lax.broadcasted_iota(jnp.int32, (BK, BQ), 1) - lax.broadcasted_iota(jnp.int32, (BK, BQ), 0)
                ok = gap >= j * BK - iq * BQ
            qs, dos = [qkv_s[rows, _head(n)] for n in mine], [by_att_s[rows, _head(n)] for n in mine]
            scores, dps = [_dot_turned(k, q) for q in qs], [_dot_turned(v, t) for t in dos]
            for x, n in enumerate(mine):
                p = jnp.exp2(scores[x] * e - lses[x])
                if masked:
                    p = jnp.where(ok, p, 0.0)
                ds = (p * (dps[x] - deltas[x])).astype(BF16)
                dv_s[i, here, :] += _dot(p.astype(BF16), dos[x])
                dk_s[i, here, :] += _dot(ds, qs[x])
                dq_s[n] += _dot(k.T, ds)

        whole = iq * BQ // BK
        if whole:
            lax.fori_loop(0, whole, lambda j, _: block(j, False), None)
        lax.fori_loop(whole, whole + BQ // BK, lambda j, _: block(j, True), None)
        for n in mine:
            dq = (dq_s[n] * scale).T.astype(BF16).astype(F32)
            by_s[rows, _head(n)] = rotated(dq, cos_ref[rows, :], sin_ref[rows, :])

    if (iq + 1) * BQ == qkv_s.shape[0]:
        for i in range(heads // group):
            dk = (dk_s[i] * scale).astype(BF16).astype(F32)
            by_s[:, _head(heads + i)] = rotated(dk, cos_ref[...], sin_ref[...])
            by_s[:, _head(heads + heads // group + i)] = dv_s[i].astype(BF16)


def p_half(ff):
    return (ff // 256 + 1) // 2 * 256 + 256


def _schedule(units, work):
    came, when, ready = 0.0, [], {}
    for u in units:
        came += u.whole.shape[0] * u.width * 2e-6
        done = START + came * PACE
        for stage, before in BEFORE.items():
            when.append((done - before * (1 + came / 100), stage, u))
        ready[u.layer, u.kind] = done
    when.sort(key=lambda e: e[0])
    order, now, work = [], 0.0, list(work)
    while when or work:
        able = work and all(ready[n] <= now for n in work[0][0]) and not [e for e in when if e[1] == "S" and (e[2].layer, e[2].kind) in work[0][0]]
        if when and (when[0][0] <= now or not able):
            order.append(when[0][1:])
            now = max(now, when.pop(0)[0])
        else:
            order.append(("run", work[0][2]))
            now += work.pop(0)[1]
    return order


def _both_passes(layers, x_ref, dy_ref, wq_b, wk_b, wv_b, o_b, g_b, u_b, d_b, cos_ref, sin_ref, *refs):
    each = len(WHOLE) + len(SAVED)
    outs = [dict(zip(WHOLE + SAVED, refs[n * each : n * each + each])) for n in range(layers)]
    refs = refs[layers * each :]
    grads = []
    half = p_half(outs[0]["g"].shape[1])
    for n in reversed(range(layers)):
        for name in GRAD_ARRAYS:
            five, refs = refs[:5], refs[5:]
            wide = five[0].shape[1]
            for part, first, columns in [("0", 0, half), ("1", half, wide - half)] if name in ("g", "u") else [("", 0, wide)]:
                grads.append(Gradient(len(grads), n, name + part, five, first, columns))
    grads.sort(key=lambda g: (-g.layer, GRADS.index(g.kind)))
    of = {(g.layer, g.kind): g for g in grads}
    (squares, p1, p2, p3, bg_s, bu_s, by_s, a_s, o_s, hm_s, bb_s, t_s, qkv_s, bq_s, mix_s, dk_s, dv_s, top_s, lse_s, wide_s, high_s,
     square_s, table_s, w_send, w_recv, load, stage_in, save, send, recv, fetching, store, meet) = refs
    tokens, d = by_s.shape
    heads, ff, three = lse_s.shape[0], p1.shape[1], qkv_s.shape[1]
    top = layers - 1
    cut = ff // 128 * 2 // 5 * 128
    hid_s, b_s, dq_s = bg_s, a_s, mix_s.at[:, pl.ds(0, HEAD), :]

    rep, way = lax.axis_index("rep"), lax.axis_index("dp")
    core, z = lax.rem(way, 2), lax.div(way, 2)
    px, py = lax.div(rep, 2), lax.rem(rep, 2)
    by_x, by_y = (1 - px) * 2 + py, px * 2 + 1 - py
    other = (rep, z * 2 + 1 - core)
    far_ways = [lax.rem(z + j, LINE) * 2 + core for j in range(1, LINE)]
    third = by_y * (1 - core) + by_x * core, by_x * (1 - core) + by_y * core
    at_end = (z == 0) | (z == LINE - 1)
    inner = jnp.logical_not(at_end)
    on = jnp.where((z == 0) | (z == 1), 1, -1)
    chip = lambda to: (rep, to * 2 + core)
    peers = [(rep, lax.rem(way + j, WAYS)) for j in range(1, WAYS)]

    held = dict(qkv=bq_s, o=bb_s, d0=p3.at[:, pl.ds(0, d // 2)], d1=p3.at[:, pl.ds(d // 2, d // 2)])
    for part in range(PARTS):
        across = pl.ds(part * cut, min(cut, ff - part * cut))
        held[f"g{part}"], held[f"u{part}"] = p1.at[:, across], p2.at[:, across]
    units, staged = [], {}
    rows = g_b.shape[1]
    for n in range(layers):
        strip = lambda i, first, wide: bu_s.at[pl.ds(i * rows, rows), pl.ds(first, wide)]
        places = dict(g=strip(n, 0, ff), u=strip(layers + n, 0, ff), qkv=strip(2 * layers, n * three, three), o=strip(2 * layers + 1, n * d, d),
                      d=t_s.at[pl.ds(n * d_b.shape[1], d_b.shape[1]), :])
        parts = dict(g=[g_b], u=[u_b], qkv=[wq_b, wk_b, wv_b], o=[o_b], d=[d_b])
        for i, name in enumerate(WHOLE):
            at = 0
            for src in parts[name]:
                to_place = places[name].at[:, pl.ds(at, src.shape[2])]
                pltpu.make_async_copy(src.at[n], to_place, stage_in.at[n, i]).start()
                at += src.shape[2]
            staged[n, name] = pltpu.make_async_copy(places[name], places[name], stage_in.at[n, i])
        for kind in KINDS:
            name, part = kind.rstrip("012"), kind[-1]
            first = int(part) * (d // 2 if name == "d" else cut) if part.isdigit() else 0
            units.append(Unit(len(units), n, kind, places[name], outs[n][name], held[kind], first))

    coming, saving = {}, {}

    def fetch(name, src, dst):
        copy = pltpu.make_async_copy(src, dst, fetching.at[FETCHED.index(name)])
        copy.start()
        coming[name] = copy

    def need(*what):
        for name in what:
            coming.pop(name).wait()

    def keep(n, name, src, dst):
        if n < top or name == "a":
            copy = pltpu.make_async_copy(src, dst, save.at[n, SAVED.index(name)])
            copy.start()
            saving[n, name] = copy

    def kept(n, *what):
        for name in what:
            if (n, name) in saving:
                saving.pop((n, name)).wait()

    def wait(ref, sem):
        pltpu.make_async_copy(ref, ref, sem).wait()

    fetch("h", x_ref, by_s)
    barrier = pltpu.get_barrier_semaphore()
    near = [(by_x, way), (by_y, way), *peers]
    for device in near:
        pl.semaphore_signal(barrier, inc=1, device_id=device, device_id_type=MESH)
    pl.semaphore_wait(barrier, len(near))


    def to(u, stage, src, dst, device):
        pltpu.make_async_remote_copy(src_ref=src, dst_ref=dst, send_sem=w_send.at[u.number, stage], recv_sem=w_recv.at[u.number, stage],
                                     device_id=device, device_id_type=MESH).start()

    def wait_for(u, quarters, *sems):
        for sem in sems:
            wait(u.bytes_of(quarters), sem)

    def begin(u):
        place = u.layer, u.kind.rstrip("012")
        if place in staged:
            staged.pop(place).wait()
        for w in far_ways:
            to(u, TO_Z, u.own(rep), u.part(way, rep), (rep, w))
        to(u, OWN, u.own(), u.part(way), other)
        pltpu.make_async_copy(u.own(), u.part(way), load.at[u.number, 1]).start()

    for u in units[:AHEAD]:
        begin(u)

    def arrived(stage, u):
        came, at_home = w_recv.at[u.number], load.at[u.number]
        if stage == "Z":
            wait_for(u, FAR, came.at[TO_Z])
            if u.number + AHEAD < len(units):
                begin(units[u.number + AHEAD])
            for w in far_ways:
                to(u, TO_X, u.part(w, rep), u.part(w, rep), (by_x, way))
                to(u, TO_Y, u.part(w, rep), u.part(w, rep), (by_y, way))
        elif stage == "P":
            wait_for(u, FAR, came.at[TO_X], came.at[TO_Y])
            for w, (place, there) in zip(far_ways, ((by_y, by_x), (by_x, by_y), third)):
                to(u, ON, u.part(w, place), u.part(w, place), (there, way))
        elif stage == "F":
            wait_for(u, FAR, came.at[ON])
            for w in far_ways:
                to(u, SWAP, u.part(w), u.part(w), other)
        else:
            wait_for(u, FAR * REPS, came.at[SWAP])
            wait_for(u, REPS, came.at[OWN], at_home.at[1])
            if u.layer < top or u.kind[0] != "d":
                pltpu.make_async_copy(u.whole.at[:, pl.ds(u.first, u.width)], u.held, at_home.at[0]).start()

    def at_hand(n, *kinds):
        for kind in kinds:
            u = units[n * len(KINDS) + KINDS.index(kind)]
            pltpu.make_async_copy(u.whole.at[:, pl.ds(u.first, u.width)], u.held, load.at[u.number, 0]).wait()

    def all_sent():
        for u in units:
            sent = w_send.at[u.number]
            wait_for(u, FAR, *(sent.at[stage] for stage in (TO_Z, TO_X, TO_Y, ON)))
            wait_for(u, FAR * REPS, sent.at[SWAP])
            wait_for(u, REPS, sent.at[OWN])


    def prepare(n):
        kept(n - 1, "b", "heads")
        if n == 0:
            need("h")
        else:
            kept(n - 1, "hid_t")
        _norm(by_s, a_s)
        keep(n, "a", a_s, outs[n]["a"])

    def project(n, first, tiles):
        if first == 0:
            at_hand(n, "qkv")

        def turn(j, here, acc):
            cos, sin = cos_ref[...], sin_ref[...]
            for half in range(2):
                t = acc[:, _head(half)].astype(BF16).astype(F32)
                t = (t * cos + pltpu.roll(t, HEAD // 2, 1) * sin).astype(BF16)
                qkv_s[:, pl.ds(pl.multiple_of((2 * j + half) * HEAD, HEAD), HEAD)] = t

        def value(j, here, acc):
            qkv_s[:, here] = acc.astype(BF16)

        turned = (three + d) // 512
        _columns(a_s, bq_s, min(tiles, turned - first), 256, turn, first)
        if first + tiles > turned:
            _columns(a_s, bq_s, first + tiles - turned, 256, value, turned)
            keep(n, "heads", qkv_s, outs[n]["heads"])

    def attention_rows(n, iq, part):
        if iq == 0:
            kept(n - 1, "att", "lse")
        _attend_rows(iq, part, qkv_s, o_s, lse_s, top_s, mix_s, HEAD**-0.5)
        if part and (iq + 1) * BQ == tokens:
            keep(n, "att", o_s, outs[n]["att"])
            keep(n, "lse", lse_s, outs[n]["lse"])

    def attended(n):
        kept(n - 1, "hm", "states")
        at_hand(n, "o")

        def add(j, here, acc):
            hm_s[:, here] = by_s[:, here] + acc.astype(BF16)

        _columns(o_s, bb_s, d // 256, 256, add)

    def prepared(n):
        keep(n, "hm", hm_s, outs[n]["hm"])
        kept(n, "a")
        _norm(hm_s, a_s)
        keep(n, "b", a_s, outs[n]["b"])
        if n == top:
            fetch("by", dy_ref, by_s)

    def gated(n, part, first, tiles):
        kinds = f"g{part}", f"u{part}"
        if first == 0:
            at_hand(n, *kinds)
        w_g, w_u = (held[kind] for kind in kinds)

        @pl.loop(first, first + tiles)
        def _(j):
            here = pl.ds(pl.multiple_of(j * 128, 128), 128)
            acc = _dot(a_s[...], jnp.concatenate([w_g[:, here], w_u[:, here]], 1))
            gate, up = acc[:, :128], acc[:, 128:]
            hidden = (jax.nn.silu(gate) * up).astype(BF16)
            across = pl.ds(pl.multiple_of(part * cut + j * 128, 128), 128)
            if n == top:
                p3[across, :] = hidden.T
            else:
                hid_s[:, across] = hidden

    def down(n, first, tiles):
        at_hand(n, "d1" if first else "d0")

        def add(j, here, acc):
            by_s[:, here] = hm_s[:, here] + acc.astype(BF16)

        _columns(hid_s, p3, tiles, 256, add, first)
        if first:
            keep(n, "states", by_s, outs[n]["states"])

    def flipped(n, part):
        first = part * cut
        _flip_out(hid_s, high_s, outs[n]["hid_t"], store, first, min(cut, ff - first))

    def last_down(part):
        if part == 0:
            need("by")
        high = high_s.shape[1]
        _rows_out(p3, by_s, high_s, of[top, "d"].whole, store, part * cut // high, min(cut * (part + 1), ff) // high)


    def remote(g, src, dst, sent, came, device):
        return pltpu.make_async_remote_copy(src_ref=src, dst_ref=dst, send_sem=send.at[g.number, sent], recv_sem=recv.at[g.number, came],
                                            device_id=device, device_id_type=MESH)

    def wait_block(g, *sems):
        for sem in sems:
            wait(g.at(g.came, 0), sem)

    def pair(g, blocks=range(LINE)):
        for there in blocks:
            sent, came = (PAIR_LAST, CAME) if there == FAR else (PAIR, PAIR)
            remote(g, g.own(there * 2 + 1 - core), g.at(g.swapped, there), sent, came, other).start()

    def added(g, jobs, after=None):
        def scoped(buf, sems):
            loads, stores, at = [], [], 0
            for parts, _ in jobs:
                mine = []
                for ref in parts:
                    mine.append(pltpu.make_async_copy(ref, buf.at[at], sems.at[at]))
                    mine[-1].start()
                    at += 1
                loads.append((mine, at - len(parts)))
            for (mine, first), (parts, to) in zip(loads, jobs):
                for c in mine:
                    c.wait()

                @pl.loop(0, g.rows // 16)
                def _(i):
                    here = pl.ds(pl.multiple_of(i * 16, 16), 16)
                    total = buf[first, here, :].astype(F32)
                    for x in range(1, len(parts)):
                        total = total + buf[first + x, here, :].astype(F32)
                    low = total.astype(BF16)
                    buf[first, here, :] = low
                    if to is g.out:
                        wide = low.astype(F32)
                        square_s[:, : g.columns] += wide * wide

                stores.append(pltpu.make_async_copy(buf.at[first], to, sems.at[first]))
                stores[-1].start()
            for x, c in enumerate(stores):
                c.wait()
                if after:
                    after(x)

        many = sum(len(parts) for parts, _ in jobs)
        pl.run_scoped(scoped, pltpu.VMEM((many, g.rows, g.columns), BF16), pltpu.SemaphoreType.DMA((many,)))

    def step_on(many):
        return jnp.clip(z + many * on, 0, LINE - 1)

    def terms(g, block):
        return [g.own(block * 2 + core), g.at(g.swapped, block)]

    def send_sum(g, block, sent, came, to):
        remote(g, g.at(g.sums, block), g.at(g.came, came - FROM_END), sent, came, chip(to)).start()

    def summed(g, *some):
        far, mid, near = step_on(3), step_on(2), step_on(1)
        job = lambda block: (terms(g, block), g.at(g.sums, block))
        send = (lambda _: send_sum(g, far, FAR_ONE, FROM_END, near)), (lambda _: send_sum(g, mid, FAR_TWO, FROM_END + 1, near))
        first, rest = "first" in some or not some, "rest" in some or not some
        if first:
            wait(g.at(g.swapped, 0, FAR), recv.at[g.number, PAIR])
        if rest:
            wait(g.at(g.swapped, 0), recv.at[g.number, CAME])
        if some:
            pl.when(z == (LINE - 1 if first else 0))(lambda: added(g, [job(far)], send[0]))
            if first:
                pl.when(at_end)(lambda: added(g, [job(mid)], send[1]))
                pl.when(at_end)(lambda: added(g, [job(near)]))
        else:
            pl.when(at_end)(lambda: added(g, [job(far), job(mid)], lambda x: send[x](x)))
            pl.when(at_end)(lambda: added(g, [job(near)]))

    def late(g):
        pl.when(at_end)(lambda: send_sum(g, step_on(1), LATE, FROM_END + 2, step_on(1)))

    def sent_far(g):
        pl.when(at_end)(lambda: wait_block(g, send.at[g.number, FAR_ONE], send.at[g.number, FAR_ONE + 1]))

    def passed(g):
        far, mid = step_on(2), step_on(1)

        def jobs():
            for x, block in enumerate((far, mid)):
                wait_block(g, recv.at[g.number, FROM_END + x])
                added(g, [(terms(g, block) + [g.at(g.came, x)], g.at(g.sums, block))],
                      lambda _, x=x, block=block: send_sum(g, block, FAR_ONE + x, FROM_MID + x, mid))

        pl.when(inner)(jobs)

    def back(g):
        end = step_on(-1)

        def jobs():
            wait_block(g, recv.at[g.number, FROM_MID])
            added(g, [(terms(g, end) + [g.at(g.came, FROM_MID - FROM_END)], g.at(g.sums, end))],
                  lambda x: send_sum(g, end, LATE, FROM_END, end))

        pl.when(inner)(jobs)

    def last(g):
        def at_inner():
            wait_block(g, recv.at[g.number, FROM_END + 2], recv.at[g.number, FROM_MID + 1])
            added(g, [(terms(g, z) + [g.at(g.came, 2), g.at(g.came, FROM_MID + 1 - FROM_END)], g.out)])

        def at_the_end():
            wait_block(g, recv.at[g.number, FROM_END])
            added(g, [(terms(g, z) + [g.at(g.came, 0)], g.out)])

        pl.when(inner)(at_inner)
        pl.when(at_end)(at_the_end)


    wqkv_s, wo_s = p1.at[:, pl.ds(0, three)], p1.at[:, pl.ds(three, d)]

    def transposed_dot(lhs, w, here):
        return _dot_turned(lhs[...], w[here, :])

    def hidden(first, many):
        def part(j, here):
            gate = _dot(b_s[...], p1[:, here])
            up = _dot(b_s[...], p2[:, here])
            by = transposed_dot(by_s, p3, here).astype(BF16).astype(F32)
            sig = jax.nn.sigmoid(gate)
            bu_s[:, here] = (by * (gate * sig)).astype(BF16)
            bg_s[:, here] = (by * up * (sig * (1 + gate * (1 - sig)))).astype(BF16)

        width = p1.shape[1]

        @pl.loop(first, min(first + many, width // 256))
        def _(j):
            part(j, pl.ds(pl.multiple_of(j * 256, 256), 256))

        if first + many > width // 256 and width % 256:
            part(width // 256, pl.ds(width // 256 * 256, width % 256))

    def project_back(w, src, dst):
        def part(j, here):
            dst[:, here] = transposed_dot(src, w, here).astype(BF16)

        _tiles(d, part)

    def by_b():
        def part(j, here):
            bb_s[:, here] = (transposed_dot(bg_s, p1, here) + transposed_dot(bu_s, p2, here)).astype(BF16)

        _tiles(d, part)


    def layer_steps(n):
        s = outs[n]
        grad = lambda kind: of[n, kind]

        def start():
            fetch("hid_t", s["hid_t"], p3)
            for name, dst in (("b", b_s), ("g", p1), ("u", p2), ("heads", qkv_s), ("lse", lse_s), ("hm", hm_s), ("att", o_s)):
                fetch(name, s[name], dst)

        def by_down():
            need("hid_t")
            _rows_out(p3, by_s, high_s, grad("d").whole, store, 0, ff // high_s.shape[1])
            fetch("d", s["d"], p3)

        def start_last():
            fetch("d", s["d"], p3)
            all_sent()
            for key in list(saving):
                kept(*key)

        def hidden_first():
            need("d")
            if n < top:
                need("b", "g", "u", "hm", "att", "heads", "lse")
            _flip(b_s, t_s)
            hidden(0, 4)

        def by_part(kind, src):
            g = grad(kind)
            _columns_out(t_s, src.at[:, g.across], wide_s, g.whole, store)

        def hidden_last():
            hidden(10, 3)
            fetch("a", s["a"], a_s)

        def by_mid():
            fetch("o", s["o"], wo_s)
            fetch("qkv", s["qkv"], wqkv_s)
            _norm_back(hm_s, bb_s, by_s)
            if n:
                fetch("h", outs[n - 1]["states"], hm_s)

        def by_o():
            _flip(o_s, t_s)
            _columns_out(t_s, by_s, wide_s, grad("o").whole, store)

        def by_att():
            need("o")
            project_back(wo_s, by_s, bb_s)

        def attention(iq):
            if iq == 0:
                dk_s[...] = jnp.zeros(dk_s.shape, F32)
                dv_s[...] = jnp.zeros(dv_s.shape, F32)
            _attend_rows_back(iq, qkv_s, o_s, bb_s, lse_s, bq_s, dq_s, dk_s, dv_s, cos_ref, sin_ref, HEAD**-0.5)

        def by_qkv():
            need("a", "qkv")
            _flip(a_s, t_s)
            _columns_out(t_s, bq_s, wide_s, grad("qkv").whole, store)

        def by_states():
            project_back(wqkv_s, bq_s, bb_s)
            need("h")
            _norm_back(hm_s, bb_s, by_s)

        f = functools.partial
        do = lambda what, *kinds: [f(what, grad(kind)) for kind in kinds]
        part = lambda kind: [f(by_part, kind, bg_s if kind[0] == "g" else bu_s)] + do(pair, kind)
        if n == top:
            steps = [start_last, hidden_first]
        else:
            steps = [start, by_down] + do(pair, "d") + [f(passed, of[n + 1, "qkv"]), hidden_first] + do(summed, "d") + [f(back, of[n + 1, "o"])]
        steps += [f(hidden, 4, 3)] + part("g0") + part("u0") + do(summed, "g0") + do(passed, "d") + [f(hidden, 7, 3)] + do(summed, "u0")
        steps += [hidden_last] + do(passed, "g0") + part("g1") + part("u1") + do(summed, "g1") + do(back, "d") + do(passed, "u0") + [by_b]
        steps += do(summed, "u1") + do(back, "g0") + do(passed, "g1") + [by_mid, by_o] + do(pair, "o") + [by_att] + do(summed, "o")
        steps += (do(late, "g0", "u0") if n == top else []) + do(back, "u0") + do(passed, "u1") + [f(attention, 0)] + do(back, "g1") + do(passed, "o")
        steps += (do(late, "g1", "u1") if n == top else []) + [f(attention, 1)] + do(back, "u1") + [by_qkv] + do(pair, "qkv")
        return steps + ([by_states] if n else []) + do(summed, "qkv") + (do(late, "o") if n == top else [])


    work = []
    f = functools.partial
    first = of[top, "d"]
    for n in range(layers):
        work += [((), 1.4, f(prepare, n)), ([(n, "qkv")], 4, f(project, n, 0, 3)), ((), 2.4, f(project, n, 3, 3))]
        work.append(((), 4, f(attention_rows, n, 0, 1)))
        for iq in range(1, tokens // BQ):
            work += [((), 4, f(attention_rows, n, iq, 0)), ((), 4, f(attention_rows, n, iq, 1))]
        work += [([(n, "o")], 3, f(attended, n)), ((), 1.4, f(prepared, n))]
        for part in range(PARTS):
            tiles = held[f"g{part}"].shape[1] // 128
            low = tiles // 2
            needs = [(n, f"g{part}"), (n, f"u{part}")]
            work += [(needs, low * 0.75 + 1, f(gated, n, part, 0, low)), ((), tiles * 0.75 / 2, f(gated, n, part, low, tiles - low))]
            if n == top:
                work.append(((), tiles * 0.35, f(last_down, part)))
                if part == PARTS - 2:
                    work.append(((), 0.1, f(pair, first, range(FAR))))
            else:
                work.append(((), tiles * 0.25, f(flipped, n, part)))
        if n < top:
            work += [([(n, f"d{part}")], 4.5, f(down, n, part * d // 512, d // 512)) for part in range(2)]
    rest = [((), 6, f(summed, first, "first")), ((), 0, f(late, first)), ((), 0, f(pair, first, [FAR]))]
    work[-1:] = [*rest[:2], work[-1], rest[2]]
    square_s[...] = jnp.zeros(square_s.shape, F32)
    for stage, what in _schedule(units, work):
        what() if stage == "run" else arrived(stage, what)
    steps = layer_steps(top)
    steps.insert(2, f(summed, first, "rest"))
    for n in reversed(range(top)):
        steps += layer_steps(n)
    for step in steps:
        step()
    end = grads[-1]
    waiting = [of[0, kind] for kind in GRADS[:5]] + [of[top, "qkv"], of[0, "o"], end]
    sent_far(of[0, "u1"])
    for g in waiting[:2]:
        late(g)
    back(of[top, "qkv"])
    passed(end)
    for kind in ("o", "qkv"):
        back(of[0, kind])
    for kind in GRADS[:6]:
        last(of[top, kind])
    sent_far(end)
    for g in waiting[2:]:
        late(g)
    for g in waiting:
        last(g)

    table_s[way] = jnp.full(table_s.shape[1:], jnp.sum(square_s[...]), F32)
    copies = []
    for j, device in enumerate(peers):
        copies.append(pltpu.make_async_remote_copy(src_ref=table_s.at[way], dst_ref=table_s.at[way], send_sem=meet.at[0, j],
                                                   recv_sem=meet.at[1, j], device_id=device, device_id_type=MESH))
        copies[-1].start()
    for copy in copies:
        copy.wait()
    total = table_s[0]
    for j in range(1, WAYS):
        total = total + table_s[j]
    squares[...] = total

    for g in grads:
        wait(g.at(g.swapped, 0, FAR), send.at[g.number, PAIR])
        wait_block(g, send.at[g.number, PAIR_LAST])
        wait_block(g, send.at[g.number, LATE])
        far = lambda g=g: wait_block(g, send.at[g.number, FAR_ONE], send.at[g.number, FAR_TWO])
        pl.when(inner)(far) if g in (end, of[0, "u1"]) else far()


def turning(tokens):
    half = HEAD // 2
    angle = jnp.arange(tokens, dtype=F32)[:, None] * THETA ** (-jnp.arange(half, dtype=F32) / half)
    cos, sin = jnp.cos(angle), jnp.sin(angle)
    return jnp.concatenate([cos, cos], 1), jnp.concatenate([-sin, sin], 1)


def both_passes(x, dy, weights):
    wq, wk, wv, wo, wg, wu, wd = weights
    layers, (tokens, wide) = wq.shape[0], x.shape
    ff, kv, heads = wg.shape[2], wk.shape[2], wide // HEAD
    three = wide + 2 * kv
    big = lambda *shape: jax.ShapeDtypeStruct(shape, BF16)
    whole = dict(qkv=big(wide, three), o=big(wide, wide), g=big(wide, ff), u=big(wide, ff), d=big(ff, wide))
    square = big(tokens, wide)
    saved = dict(a=square, heads=big(tokens, three), att=square, lse=jax.ShapeDtypeStruct((heads, tokens), F32), hm=square, b=square,
                 states=square, hid_t=big(ff, tokens))
    outs = [*whole.values(), *(saved[name] for name in SAVED)] * layers
    where = {}
    for n in reversed(range(layers)):
        for kind in GRAD_ARRAYS:
            rows, columns = whole[kind].shape
            part = rows // WAYS
            outs += [whole[kind], *[big(rows // 2, columns)] * 2, big(part * (CAME - FROM_END), columns), big(part, columns)]
            where[n, kind] = len(outs) - 1
    vm = lambda *shape: pltpu.VMEM(shape, BF16)
    f32 = lambda *shape: pltpu.VMEM(shape, F32)
    sems = lambda *shape: pltpu.SemaphoreType.DMA(shape)
    units, count = layers * len(KINDS), layers * len(GRADS)
    got = pl.pallas_call(
        functools.partial(_both_passes, layers),
        in_specs=[EVERY] * 9 + [INNER] * 2,
        out_specs=[EVERY] * len(outs) + [INNER],
        out_shape=[*outs, jax.ShapeDtypeStruct((8, 128), F32)],
        scratch_shapes=[vm(wide, ff), vm(wide, ff), vm(ff, wide), vm(tokens, ff), vm(tokens, ff), *[vm(tokens, wide)] * 6, vm(tokens, three),
                        vm(tokens, three), f32(heads, HEAD + 8, BQ), *[f32(kv // HEAD, tokens, HEAD)] * 2, f32(heads, BQ), f32(heads, tokens),
                        vm(2, wide, 256), vm(2, ff // 10, wide), f32(16, ff), f32(WAYS, 8, 128),
                        sems(units, OWN + 1), sems(units, OWN + 1), sems(units, 2), sems(layers, len(WHOLE)), sems(layers, len(SAVED)),
                        sems(count, PAIR_LAST + 1), sems(count, CAME + 1), sems(len(FETCHED)), sems(2), sems(2, WAYS - 1)],
        compiler_params=pltpu.CompilerParams(collective_id=0, has_side_effects=True, vmem_limit_bytes=67043328),
        cost_estimate=pl.CostEstimate(flops=270 * 10**9, bytes_accessed=6 * 10**8, transcendentals=10**7),
        name="both_passes",
    )(x, dy, *weights, *turning(tokens))
    return [{kind: got[where[n, kind]] for kind in GRAD_ARRAYS} for n in range(layers)], got[-1][0, 0]


from jax.sharding import PartitionSpec as P


def adamw(w, m, v, g):
    m = 0.9 * m + 0.1 * g
    v = 0.95 * v + 0.05 * g * g
    step = m * lax.rsqrt(v + 1e-8) + 0.1 * w
    return (w - 0.02 * step).astype(BF16), m, v


def solution(mesh):
    def step(x, dy, *arrays):
        weights, m, v = (arrays[i : i + 7] for i in (0, 7, 14))
        d, kv = weights[0].shape[2], weights[1].shape[2]
        parts, squares = both_passes(x[0], dy[0], weights)
        count = WAYS * sum(w.size for w in weights)
        factor = jnp.minimum(1.0, 0.5 * lax.rsqrt(squares / count + 1e-30))
        split = lambda p: (p["qkv"][:, :d], p["qkv"][:, d : d + kv], p["qkv"][:, d + kv :], p["o"], p["g"], p["u"], p["d"])
        gradients = [jnp.stack(g).astype(F32) * factor for g in zip(*(split(p) for p in parts))]
        new = [adamw(w.astype(F32), m, v, g) for w, m, v, g in zip(weights, m, v, gradients, strict=True)]
        return tuple(one[which] for which in range(3) for one in new)

    states, cut = P(("rep", "dp"), None, None), P(None, "dp", None)
    return jax.shard_map(
        step,
        mesh=mesh,
        in_specs=(states, states) + (cut,) * 21,
        out_specs=(P("rep", "dp", None),) * 21,
        check_vma=False,
    )
```

```python
import functools
import math

import jax
import jax.numpy as jnp
import numpy as np
from jax import lax
from jax.experimental import pallas as pl
from jax.experimental.pallas import tpu as pltpu
from jax.sharding import PartitionSpec as P

NEG = -1e30
HIDDEN = 2 * NEG
LOG2E = 1.4426950408889634


def _dot(a, b):
    return jnp.dot(a, b, preferred_element_type=jnp.float32)


def _dot_turned(a, b):
    return lax.dot_general(a, b, (((1,), (1,)), ((), ())), preferred_element_type=jnp.float32)


HEAD = 128
THETA = 10000
F32, BF16 = jnp.float32, jnp.bfloat16
MESH = pl.DeviceIdType.MESH
REPS, WAYS, LINE = 4, 8, 4
TILE, LANES, PACK = 256, 128, 16
BQ, BK = 512, 256
TO_Z, TO_X, TO_Y, ON, SWAP, OWN = range(6)
FAR = LINE - 1
START, PACE, BEFORE = 24.0, 3.0, dict(Z=24, P=14, F=6, S=0)
SHIFT = {("S", "q"): -3, ("F", "o"): 3}
AHEAD = 2
KINDS = ("qkv0", "qkv1", "o", "g0", "u0", "g1", "u1", "g2", "u2", "d0", "d1")
PARTS = 3
NAMES = ["wq", "wk", "wv", "wo", "w_gate", "w_up", "w_down"]
WHOLE = ["qkv", "o", "g", "u", "d"]
SAVED = ["a", "heads", "att", "lse", "hm", "b", "states", "hid_t"]
GRADS = ["d", "g0", "u0", "g1", "u1", "o", "qkv"]
GRAD_ARRAYS = ["d", "g", "u", "o", "qkv"]
FETCHED = ["by", "hid_t", "b", "d", "g", "u", "hm", "att", "a", "heads", "lse", "o", "qkv", "h"]
AT_ONCE = 4
PAIR, FAR_ONE, FAR_TWO, LATE, PAIR_LAST = range(5)
FROM_END, FROM_MID, CAME = 1, 4, 6
EVERY = pl.BlockSpec(memory_space=pl.ANY)
INNER = pl.BlockSpec(memory_space=pltpu.VMEM)


class Unit:
    def __init__(self, number, layer, kind, block, whole, held, first):
        self.number, self.layer, self.kind, self.block, self.whole, self.held = number, layer, kind, block, whole, held
        self.first, self.width, self.rows = first, held.shape[1], whole.shape[0] // WAYS
        self.by_columns = self.rows // REPS % PACK != 0

    def cut(self, ref, base, place):
        part = (self.width if self.by_columns else self.rows) // REPS
        if place is None:
            return ref.at[pl.ds(pl.multiple_of(base, 8), self.rows), pl.ds(self.first, self.width)]
        if self.by_columns:
            return ref.at[pl.ds(pl.multiple_of(base, 8), self.rows), pl.ds(pl.multiple_of(self.first + place * part, LANES), part)]
        return ref.at[pl.ds(pl.multiple_of(base + place * part, part), part), pl.ds(self.first, self.width)]

    def own(self, place=None):
        return self.cut(self.block, 0, place)

    def part(self, way, place=None):
        return self.cut(self.whole, way * self.rows, place)

    def bytes_of(self, quarters):
        if self.by_columns:
            return self.whole.at[pl.ds(0, -(-quarters // REPS) * self.rows), pl.ds(self.first, min(quarters, REPS) * self.width // REPS)]
        return self.whole.at[pl.ds(0, quarters * self.rows // REPS), pl.ds(self.first, self.width)]


def _norm(src, dst, rows=LANES):
    @pl.loop(0, src.shape[0] // rows)
    def _(i):
        here = pl.ds(pl.multiple_of(i * rows, rows), rows)
        wide = src[here, :].astype(F32)
        scale = lax.rsqrt(jnp.mean(wide * wide, -1, keepdims=True) + 1e-6)
        dst[here, :] = (wide * scale).astype(BF16)


def _columns(lhs, w, tiles, width, use, first=0):
    @pl.loop(first, first + tiles)
    def _(j):
        here = pl.ds(pl.multiple_of(j * width, width), width)
        use(j, here, _dot(lhs[...], w[:, here]))


def _head(n):
    return slice(n * HEAD, (n + 1) * HEAD)


def _attend_rows(iq, part, qkv_s, o_s, lse_s, top_s, mix_s, scale):
    heads, d = top_s.shape[0], HEAD
    group = 2 * heads // (qkv_s.shape[1] // HEAD - heads)
    e = scale * LOG2E
    rows = pl.ds(iq * BQ, BQ)
    whole = iq * BQ // BK
    if part == 0 or not whole:
        top_s[...] = jnp.full(top_s.shape, NEG, F32)
        mix_s[...] = jnp.zeros(mix_s.shape, F32)
    ones = jnp.ones((8, BK), BF16)

    def block(j, masked):
        here = pl.ds(pl.multiple_of(j * BK, BK), BK)
        scores = [_dot_turned(qkv_s[here, _head(heads + n // group)], qkv_s[rows, _head(n)]) for n in range(heads)]
        if masked:
            gap = lax.broadcasted_iota(jnp.int32, (BK, BQ), 1) - lax.broadcasted_iota(jnp.int32, (BK, BQ), 0)
            ok = gap >= j * BK - iq * BQ
        weights, keeps = [], []
        for n, s in enumerate(scores):
            if masked:
                s = jnp.where(ok, s, HIDDEN)
            old = top_s[n : n + 1, :]
            top = jnp.maximum(old, s.max(axis=0, keepdims=True))
            top_s[n : n + 1, :] = top
            weights.append(jnp.exp2((s - top) * e).astype(BF16))
            keeps.append(jnp.exp2((old - top) * e))
        for n, (p, keep) in enumerate(zip(weights, keeps)):
            values = jnp.concatenate([qkv_s[here, _head(heads + (heads + n) // group)].T, ones], axis=0)
            mix_s[n] = mix_s[n] * keep + _dot(values, p)

    if part == 0:
        lax.fori_loop(0, whole, lambda j, _: block(j, False), None)
        return
    lax.fori_loop(whole, whole + BQ // BK, lambda j, _: block(j, True), None)
    for n in range(heads):
        total = mix_s[n, d : d + 1, :]
        o_s[rows, _head(n)] = (mix_s[n, :d, :] * (1 / total)).T.astype(BF16)
        lse_s[n : n + 1, rows] = top_s[n : n + 1, :] * scale + jnp.log(total)


def _flip(src, dst, first=0, width=None, rows=LANES):
    across = pl.ds(first, width or src.shape[1])

    @pl.loop(0, src.shape[0] // rows)
    def _(i):
        here = pl.ds(pl.multiple_of(i * rows, rows), rows)
        dst[across, here] = src[here, across].T


def _flip_out(src, out_s, dst, sems, first, width):
    def copy(i, slot):
        return pltpu.make_async_copy(out_s.at[slot, pl.ds(0, LANES), :], dst.at[pl.ds(pl.multiple_of(i * LANES, LANES), LANES), :], sems.at[slot])

    start, end = first // LANES, (first + width) // LANES

    @pl.loop(start, end)
    def _(i):
        slot = lax.rem(i, 2)

        @pl.when(i >= start + 2)
        def _():
            copy(i - 2, slot).wait()

        out_s[slot, :LANES, :] = src[:, pl.ds(pl.multiple_of(i * LANES, LANES), LANES)].T
        copy(i, slot).start()

    for i in (end - 2, end - 1):
        copy(i, i % 2).wait()


def _rows_out(lhs, rhs, out_s, dst, sems, first, last):
    high = out_s.shape[1]

    def copy(i, slot):
        return pltpu.make_async_copy(out_s.at[slot], dst.at[pl.ds(pl.multiple_of(i * high, 8), high), :], sems.at[slot])

    @pl.loop(first, last)
    def _(i):
        slot = lax.rem(i, 2)

        @pl.when(i >= first + 2)
        def _():
            copy(i - 2, slot).wait()

        out_s[slot] = _dot(lhs[pl.ds(pl.multiple_of(i * high, 8), high), :], rhs[...]).astype(BF16)
        copy(i, slot).start()

    for i in (last - 2, last - 1):
        copy(i, i % 2).wait()


class Gradient:
    def __init__(self, number, layer, kind, refs, first, columns):
        self.number, self.layer, self.kind, self.first, self.columns = number, layer, kind, first, columns
        whole, self.swapped, self.sums, self.came, out = refs
        self.rows = out.shape[0]
        across = pl.ds(first, columns)
        self.whole, self.out = whole.at[:, across], out.at[:, across]
        self.across = across

    def at(self, ref, block, many=1):
        return ref.at[pl.ds(pl.multiple_of(block * self.rows, 8), many * self.rows), self.across]

    def own(self, block):
        return self.whole.at[pl.ds(pl.multiple_of(block * self.rows, 8), self.rows), :]


def _tiles(width, use, size=TILE):
    @pl.loop(0, width // size)
    def _(j):
        use(j, pl.ds(pl.multiple_of(j * size, size), size))

    if width % size:
        use(width // size, pl.ds(width // size * size, width % size))


def _columns_out(lhs, rhs, out_s, dst, sems):
    width = rhs.shape[1]
    steps = -(-width // TILE)

    def copy(j, here, slot):
        return pltpu.make_async_copy(out_s.at[slot, :, pl.ds(0, here.size)], dst.at[:, here], sems.at[slot])

    def part(j, here):
        slot = lax.rem(j, 2) if not isinstance(j, int) else j % 2
        before = pl.ds(pl.multiple_of((j - 2) * TILE, TILE), TILE)
        if isinstance(j, int):
            copy(j - 2, before, slot).wait()
        else:
            pl.when(j >= 2)(lambda: copy(j - 2, before, slot).wait())
        out_s[slot, :, : here.size] = _dot(lhs[...], rhs[:, here]).astype(BF16)
        copy(j, here, slot).start()

    _tiles(width, part)
    for j in (steps - 2, steps - 1):
        copy(j, pl.ds(j * TILE, min(TILE, width - j * TILE)), j % 2).wait()


def _norm_back(h, by_normed, by, first=False, rows=LANES):
    @pl.loop(0, by.shape[0] // rows)
    def _(i):
        here = pl.ds(pl.multiple_of(i * rows, rows), rows)
        wide, grad = h[here, :].astype(F32), by_normed[here, :].astype(F32)
        scale = lax.rsqrt(jnp.mean(wide * wide, -1, keepdims=True) + 1e-6)
        along = jnp.mean(wide * grad, -1, keepdims=True)
        by[here, :] = by[here, :] + (scale * grad - wide * (scale * scale * scale * along)).astype(BF16)


def _attend_rows_back(iq, qkv_s, att_s, by_att_s, lse_s, by_s, dq_s, dk_s, dv_s, cos_ref, sin_ref, scale):
    heads, d = lse_s.shape[0], HEAD
    group = 2 * heads // (qkv_s.shape[1] // HEAD - heads)
    e = scale * LOG2E
    rows = pl.ds(iq * BQ, BQ)
    dq_s[...] = jnp.zeros(dq_s.shape, F32)
    rotated = lambda t, c, s: (t * c - pltpu.roll(t, HEAD // 2, 1) * s).astype(BF16)

    for i in range(heads // group):
        mine = range(i * group, (i + 1) * group)
        lses = [lse_s[n : n + 1, rows] * LOG2E for n in mine]
        deltas = [(by_att_s[rows, _head(n)].astype(F32) * att_s[rows, _head(n)].astype(F32)).T.sum(axis=0, keepdims=True) for n in mine]

        def block(j, masked):
            here = pl.ds(pl.multiple_of(j * BK, BK), BK)
            k, v = qkv_s[here, _head(heads + i)], qkv_s[here, _head(heads + heads // group + i)]
            if masked:
                gap = lax.broadcasted_iota(jnp.int32, (BK, BQ), 1) - lax.broadcasted_iota(jnp.int32, (BK, BQ), 0)
                ok = gap >= j * BK - iq * BQ
            qs, dos = [qkv_s[rows, _head(n)] for n in mine], [by_att_s[rows, _head(n)] for n in mine]
            scores, dps = [_dot_turned(k, q) for q in qs], [_dot_turned(v, t) for t in dos]
            for x, n in enumerate(mine):
                p = jnp.exp2(scores[x] * e - lses[x])
                if masked:
                    p = jnp.where(ok, p, 0.0)
                ds = (p * (dps[x] - deltas[x])).astype(BF16)
                dv_s[i, here, :] += _dot(p.astype(BF16), dos[x])
                dk_s[i, here, :] += _dot(ds, qs[x])
                dq_s[n] += _dot(k.T, ds)

        whole = iq * BQ // BK
        if whole:
            lax.fori_loop(0, whole, lambda j, _: block(j, False), None)
        lax.fori_loop(whole, whole + BQ // BK, lambda j, _: block(j, True), None)
        for n in mine:
            dq = (dq_s[n] * scale).T.astype(BF16).astype(F32)
            by_s[rows, _head(n)] = rotated(dq, cos_ref[rows, :], sin_ref[rows, :])

    if (iq + 1) * BQ == qkv_s.shape[0]:
        for i in range(heads // group):
            dk = (dk_s[i] * scale).astype(BF16).astype(F32)
            by_s[:, _head(heads + i)] = rotated(dk, cos_ref[...], sin_ref[...])
            by_s[:, _head(heads + heads // group + i)] = dv_s[i].astype(BF16)


def p_half(ff):
    return (ff // TILE + 1) // 2 * TILE + TILE


def _schedule(units, work):
    came, when, ready = 0.0, [], {}
    for u in units:
        came += u.whole.shape[0] * u.width * 2e-6
        done = START + came * PACE
        for stage, before in BEFORE.items():
            shift = SHIFT.get((stage, u.kind[0]), 0) * (u.layer > 0)
            when.append((done - before * (1 + came / 100) + shift, stage, u))
        ready[u.layer, u.kind] = done
    when.sort(key=lambda e: e[0])
    order, now, work = [], 0.0, list(work)
    while when or work:
        able = work and all(ready[n] <= now for n in work[0][0]) and not [e for e in when if e[1] == "S" and (e[2].layer, e[2].kind) in work[0][0]]
        if when and (when[0][0] <= now or not able):
            order.append(when[0][1:])
            now = max(now, when.pop(0)[0])
        else:
            order.append(("run", work[0][2]))
            now += work.pop(0)[1]
    return order


def _both_passes(layers, x_ref, dy_ref, wq_b, wk_b, wv_b, o_b, g_b, u_b, d_b, turns_ref, *refs):
    each = len(WHOLE) + len(SAVED)
    outs = [dict(zip(WHOLE + SAVED, refs[n * each : n * each + each])) for n in range(layers)]
    refs = refs[layers * each :]
    grads = []
    half = p_half(outs[0]["g"].shape[1])
    for n in reversed(range(layers)):
        for name in GRAD_ARRAYS:
            five, refs = refs[:5], refs[5:]
            wide = five[0].shape[1]
            for part, first, columns in [("0", 0, half), ("1", half, wide - half)] if name in ("g", "u") else [("", 0, wide)]:
                grads.append(Gradient(len(grads), n, name + part, five, first, columns))
    grads.sort(key=lambda g: (-g.layer, GRADS.index(g.kind)))
    of = {(g.layer, g.kind): g for g in grads}
    (squares, p1, p2, p3, bg_s, bu_s, by_s, a_s, o_s, hm_s, bb_s, t_s, qkv_s, bq_s, mix_s, dk_s, dv_s, top_s, lse_s, wide_s, high_s,
     square_s, table_s, cos_ref, sin_ref, w_send, w_recv, load, stage_in, save, send, recv, fetching, store, meet) = refs
    tokens, d = by_s.shape
    heads, ff, three = lse_s.shape[0], p1.shape[1], qkv_s.shape[1]
    top = layers - 1
    cut = ff // LANES * 2 // 5 * LANES
    hid_s, b_s, dq_s = bg_s, a_s, mix_s.at[:, pl.ds(0, HEAD), :]

    rep, way = lax.axis_index("rep"), lax.axis_index("dp")
    core, z = lax.rem(way, 2), lax.div(way, 2)
    px, py = lax.div(rep, 2), lax.rem(rep, 2)
    by_x, by_y = (1 - px) * 2 + py, px * 2 + 1 - py
    other = (rep, z * 2 + 1 - core)
    far_ways = [lax.rem(z + j, LINE) * 2 + core for j in range(1, LINE)]
    third = by_y * (1 - core) + by_x * core, by_x * (1 - core) + by_y * core
    at_end = (z == 0) | (z == LINE - 1)
    inner = jnp.logical_not(at_end)
    on = jnp.where((z == 0) | (z == 1), 1, -1)
    chip = lambda to: (rep, to * 2 + core)
    peers = [(rep, lax.rem(way + j, WAYS)) for j in range(1, WAYS)]

    widths = dict(qkv=three // 2, d=d // 2)
    held = dict(qkv0=bq_s.at[:, pl.ds(0, three // 2)], qkv1=bq_s.at[:, pl.ds(three // 2, three // 2)], o=bb_s, d0=p3.at[:, pl.ds(0, d // 2)], d1=p3.at[:, pl.ds(d // 2, d // 2)])
    for part in range(PARTS):
        across = pl.ds(part * cut, min(cut, ff - part * cut))
        held[f"g{part}"], held[f"u{part}"] = p1.at[:, across], p2.at[:, across]
    units, staged = [], {}
    rows = g_b.shape[1]
    for n in range(layers):
        strip = lambda i, first, wide: bu_s.at[pl.ds(i * rows, rows), pl.ds(first, wide)]
        places = dict(g=strip(n, 0, ff), u=strip(layers + n, 0, ff), qkv=strip(2 * layers, n * three, three), o=strip(2 * layers + 1, n * d, d),
                      d=t_s.at[pl.ds(n * d_b.shape[1], d_b.shape[1]), :])
        parts = dict(g=[g_b], u=[u_b], qkv=[wq_b, wk_b, wv_b], o=[o_b], d=[d_b])
        for i, name in enumerate(WHOLE):
            at = 0
            for src in parts[name]:
                to_place = places[name].at[:, pl.ds(at, src.shape[2])]
                pltpu.make_async_copy(src.at[n], to_place, stage_in.at[n, i]).start()
                at += src.shape[2]
            staged[n, name] = pltpu.make_async_copy(places[name], places[name], stage_in.at[n, i])
        for kind in KINDS:
            name, part = kind.rstrip("012"), kind[-1]
            first = int(part) * widths.get(name, cut) if part.isdigit() else 0
            units.append(Unit(len(units), n, kind, places[name], outs[n][name], held[kind], first))

    coming, saving = {}, {}

    def fetch(name, src, dst):
        copy = pltpu.make_async_copy(src, dst, fetching.at[FETCHED.index(name)])
        copy.start()
        coming[name] = copy

    def need(*what):
        for name in what:
            coming.pop(name).wait()

    def keep(n, name, src, dst):
        if n < top or name == "a":
            copy = pltpu.make_async_copy(src, dst, save.at[n, SAVED.index(name)])
            copy.start()
            saving[n, name] = copy

    def kept(n, *what):
        for name in what:
            if (n, name) in saving:
                saving.pop((n, name)).wait()

    def wait(ref, sem):
        pltpu.make_async_copy(ref, ref, sem).wait()

    fetch("h", x_ref, by_s)

    @pl.loop(0, tokens // turns_ref.shape[1])
    def _(i):
        near_cos, near_sin, near_signed = (turns_ref[x] for x in range(3))
        far_cos, far_sin, far_signed = (turns_ref[3 + x, pl.ds(i, 1), :] for x in range(3))
        here = pl.ds(pl.multiple_of(i * turns_ref.shape[1], 8), turns_ref.shape[1])
        cos_ref[here, :] = far_cos * near_cos - far_sin * near_sin
        sin_ref[here, :] = far_signed * near_cos + far_cos * near_signed

    barrier = pltpu.get_barrier_semaphore()
    near = [(by_x, way), (by_y, way), *peers]
    for device in near:
        pl.semaphore_signal(barrier, inc=1, device_id=device, device_id_type=MESH)
    pl.semaphore_wait(barrier, len(near))


    def to(u, stage, src, dst, device):
        pltpu.make_async_remote_copy(src_ref=src, dst_ref=dst, send_sem=w_send.at[u.number, stage], recv_sem=w_recv.at[u.number, stage],
                                     device_id=device, device_id_type=MESH).start()

    def wait_for(u, quarters, *sems):
        for sem in sems:
            wait(u.bytes_of(quarters), sem)

    def begin(u):
        place = u.layer, u.kind.rstrip("012")
        if place in staged:
            staged.pop(place).wait()
        for w in far_ways:
            to(u, TO_Z, u.own(rep), u.part(way, rep), (rep, w))
        to(u, OWN, u.own(), u.part(way), other)
        pltpu.make_async_copy(u.own(), u.part(way), load.at[u.number, 1]).start()

    for u in units[:AHEAD]:
        begin(u)

    def arrived(stage, u):
        came, at_home = w_recv.at[u.number], load.at[u.number]
        if stage == "Z":
            wait_for(u, FAR, came.at[TO_Z])
            if u.number + AHEAD < len(units):
                begin(units[u.number + AHEAD])
            for w in far_ways:
                to(u, TO_X, u.part(w, rep), u.part(w, rep), (by_x, way))
                to(u, TO_Y, u.part(w, rep), u.part(w, rep), (by_y, way))
        elif stage == "P":
            wait_for(u, FAR, came.at[TO_X], came.at[TO_Y])
            for w, (place, there) in zip(far_ways, ((by_y, by_x), (by_x, by_y), third)):
                to(u, ON, u.part(w, place), u.part(w, place), (there, way))
        elif stage == "F":
            wait_for(u, FAR, came.at[ON])
            for w in far_ways:
                to(u, SWAP, u.part(w), u.part(w), other)
        else:
            wait_for(u, FAR * REPS, came.at[SWAP])
            wait_for(u, REPS, came.at[OWN], at_home.at[1])
            if u.layer < top or u.kind[0] != "d":
                pltpu.make_async_copy(u.whole.at[:, pl.ds(u.first, u.width)], u.held, at_home.at[0]).start()

    def at_hand(n, *kinds):
        for kind in kinds:
            u = units[n * len(KINDS) + KINDS.index(kind)]
            pltpu.make_async_copy(u.whole.at[:, pl.ds(u.first, u.width)], u.held, load.at[u.number, 0]).wait()

    def all_sent():
        for u in units:
            sent = w_send.at[u.number]
            wait_for(u, FAR, *(sent.at[stage] for stage in (TO_Z, TO_X, TO_Y, ON)))
            wait_for(u, FAR * REPS, sent.at[SWAP])
            wait_for(u, REPS, sent.at[OWN])


    def prepare(n):
        kept(n - 1, "b", "heads")
        if n == 0:
            need("h")
        else:
            kept(n - 1, "hid_t")
        _norm(by_s, a_s)
        keep(n, "a", a_s, outs[n]["a"])

    def project(n, first, tiles):
        if first == 0:
            at_hand(n, "qkv0", "qkv1")

        def turn(j, here, acc):
            cos, sin = cos_ref[...], sin_ref[...]
            for half in range(2):
                t = acc[:, _head(half)].astype(BF16).astype(F32)
                t = (t * cos + pltpu.roll(t, HEAD // 2, 1) * sin).astype(BF16)
                qkv_s[:, pl.ds(pl.multiple_of((2 * j + half) * HEAD, HEAD), HEAD)] = t

        def value(j, here, acc):
            qkv_s[:, here] = acc.astype(BF16)

        turned = (three + d) // 512
        _columns(a_s, bq_s, min(tiles, turned - first), TILE, turn, first)
        if first + tiles > turned:
            _columns(a_s, bq_s, first + tiles - turned, TILE, value, turned)
            keep(n, "heads", qkv_s, outs[n]["heads"])

    def attention_rows(n, iq, part):
        if iq == 0:
            kept(n - 1, "att", "lse")
        _attend_rows(iq, part, qkv_s, o_s, lse_s, top_s, mix_s, HEAD**-0.5)
        if part and (iq + 1) * BQ == tokens:
            keep(n, "att", o_s, outs[n]["att"])
            keep(n, "lse", lse_s, outs[n]["lse"])

    def attended(n):
        kept(n - 1, "hm", "states")
        at_hand(n, "o")

        def add(j, here, acc):
            hm_s[:, here] = by_s[:, here] + acc.astype(BF16)

        _columns(o_s, bb_s, d // TILE, TILE, add)

    def prepared(n):
        keep(n, "hm", hm_s, outs[n]["hm"])
        kept(n, "a")
        _norm(hm_s, a_s)
        keep(n, "b", a_s, outs[n]["b"])
        if n == top:
            fetch("by", dy_ref, by_s)

    def gated(n, part, first, tiles):
        kinds = f"g{part}", f"u{part}"
        if first == 0:
            at_hand(n, *kinds)
        w_g, w_u = (held[kind] for kind in kinds)

        @pl.loop(first, first + tiles)
        def _(j):
            here = pl.ds(pl.multiple_of(j * LANES, LANES), LANES)
            acc = _dot(a_s[...], jnp.concatenate([w_g[:, here], w_u[:, here]], 1))
            gate, up = acc[:, :LANES], acc[:, LANES:]
            hidden = (jax.nn.silu(gate) * up).astype(BF16)
            across = pl.ds(pl.multiple_of(part * cut + j * LANES, LANES), LANES)
            if n == top:
                p3[across, :] = hidden.T
            else:
                hid_s[:, across] = hidden

    def down(n, first, tiles):
        at_hand(n, "d1" if first else "d0")

        def add(j, here, acc):
            by_s[:, here] = hm_s[:, here] + acc.astype(BF16)

        _columns(hid_s, p3, tiles, TILE, add, first)
        if first:
            keep(n, "states", by_s, outs[n]["states"])

    def flipped(n, part):
        first = part * cut
        _flip_out(hid_s, high_s, outs[n]["hid_t"], store, first, min(cut, ff - first))

    def last_down(part):
        if part == 0:
            need("by")
        high = high_s.shape[1]
        _rows_out(p3, by_s, high_s, of[top, "d"].whole, store, part * cut // high, min(cut * (part + 1), ff) // high)


    def remote(g, src, dst, sent, came, device):
        return pltpu.make_async_remote_copy(src_ref=src, dst_ref=dst, send_sem=send.at[g.number, sent], recv_sem=recv.at[g.number, came],
                                            device_id=device, device_id_type=MESH)

    def wait_block(g, *sems):
        for sem in sems:
            wait(g.at(g.came, 0), sem)

    def pair(g, blocks=range(LINE)):
        for there in blocks:
            sent, came = (PAIR_LAST, CAME) if there == FAR else (PAIR, PAIR)
            remote(g, g.own(there * 2 + 1 - core), g.at(g.swapped, there), sent, came, other).start()

    def added(g, jobs, after=None):
        def scoped(buf, sems):
            loads, stores, at = [], [], 0
            for parts, _ in jobs:
                mine = []
                for ref in parts:
                    mine.append(pltpu.make_async_copy(ref, buf.at[at], sems.at[at]))
                    mine[-1].start()
                    at += 1
                loads.append((mine, at - len(parts)))
            for (mine, first), (parts, to) in zip(loads, jobs):
                for c in mine:
                    c.wait()

                @pl.loop(0, g.rows // PACK)
                def _(i):
                    here = pl.ds(pl.multiple_of(i * PACK, PACK), PACK)
                    total = buf[first, here, :].astype(F32)
                    for x in range(1, len(parts)):
                        total = total + buf[first + x, here, :].astype(F32)
                    low = total.astype(BF16)
                    buf[first, here, :] = low

                stores.append(pltpu.make_async_copy(buf.at[first], to, sems.at[first]))
                stores[-1].start()
            for x, c in enumerate(stores):
                c.wait()
                if after:
                    after(x)

        many = sum(len(parts) for parts, _ in jobs)
        pl.run_scoped(scoped, pltpu.VMEM((many, g.rows, g.columns), BF16), pltpu.SemaphoreType.DMA((many,)))

    def step_on(many):
        return jnp.clip(z + many * on, 0, LINE - 1)

    def terms(g, block):
        return [g.own(block * 2 + core), g.at(g.swapped, block)]

    def send_sum(g, block, sent, came, to):
        remote(g, g.at(g.sums, block), g.at(g.came, came - FROM_END), sent, came, chip(to)).start()

    def summed(g, *some):
        far, mid, near = step_on(3), step_on(2), step_on(1)
        job = lambda block: (terms(g, block), g.at(g.sums, block))
        send = (lambda _: send_sum(g, far, FAR_ONE, FROM_END, near)), (lambda _: send_sum(g, mid, FAR_TWO, FROM_END + 1, near))
        first, rest = "first" in some or not some, "rest" in some or not some
        if first:
            wait(g.at(g.swapped, 0, FAR), recv.at[g.number, PAIR])
        if rest:
            wait(g.at(g.swapped, 0), recv.at[g.number, CAME])
        if some:
            pl.when(z == (LINE - 1 if first else 0))(lambda: added(g, [job(far)], send[0]))
            if first:
                pl.when(at_end)(lambda: added(g, [job(mid)], send[1]))
                pl.when(at_end)(lambda: added(g, [job(near)]))
        else:
            pl.when(at_end)(lambda: added(g, [job(far), job(mid)], lambda x: send[x](x)))
            pl.when(at_end)(lambda: added(g, [job(near)]))

    def late(g):
        pl.when(at_end)(lambda: send_sum(g, step_on(1), LATE, FROM_END + 2, step_on(1)))

    def sent_far(g):
        pl.when(at_end)(lambda: wait_block(g, send.at[g.number, FAR_ONE], send.at[g.number, FAR_ONE + 1]))

    def passed(g):
        far, mid = step_on(2), step_on(1)

        def jobs():
            for x, block in enumerate((far, mid)):
                wait_block(g, recv.at[g.number, FROM_END + x])
                added(g, [(terms(g, block) + [g.at(g.came, x)], g.at(g.sums, block))],
                      lambda _, x=x, block=block: send_sum(g, block, FAR_ONE + x, FROM_MID + x, mid))

        pl.when(inner)(jobs)

    def back(g):
        end = step_on(-1)

        def jobs():
            wait_block(g, recv.at[g.number, FROM_MID])
            added(g, [(terms(g, end) + [g.at(g.came, FROM_MID - FROM_END)], g.at(g.sums, end))],
                  lambda x: send_sum(g, end, LATE, FROM_END, end))

        pl.when(inner)(jobs)

    def last(gs):
        def places(k):
            g = gs[k]
            pool, first = (p3, k % 2) if g.rows > LANES else ((p1, p2)[k // 2 % 2], k % 2)
            return [pool.at[pl.ds((first * LINE + i) * g.rows, g.rows), pl.ds(0, g.columns)] for i in range(LINE)]

        def copies(k):
            g = gs[k]
            parts = terms(g, z) + [g.at(g.came, FROM_MID + 1 - FROM_END), g.at(g.came, jnp.where(at_end, 0, 2))]
            return [pltpu.make_async_copy(src, dst, load.at[k % AT_ONCE * LINE + i, 0]) for i, (src, dst) in enumerate(zip(parts, places(k)))]

        def out(k):
            return pltpu.make_async_copy(places(k)[0], gs[k].out, load.at[k % AT_ONCE, 1])

        def start(k):
            came = recv.at[gs[k].number]
            own, swapped, mid, end = copies(k)

            @pl.when(inner)
            def _():
                wait_block(gs[k], came.at[FROM_END + 2], came.at[FROM_MID + 1])
                mid.start()

            pl.when(at_end)(lambda: wait_block(gs[k], came.at[FROM_END]))
            for c in (own, swapped, end):
                c.start()

        def finish(k):
            own, swapped, mid, end = copies(k)
            for c in (own, swapped, end):
                c.wait()
            pl.when(inner)(mid.wait)
            own, swapped, mid, end = places(k)
            across = pl.ds(0, gs[k].columns)

            @pl.loop(0, gs[k].rows // PACK)
            def _(i):
                here = pl.ds(pl.multiple_of(i * PACK, PACK), PACK)
                total = own[here, :].astype(F32) + swapped[here, :].astype(F32) + end[here, :].astype(F32)
                low = jnp.where(inner, total + mid[here, :].astype(F32), total).astype(BF16)
                own[here, :] = low
                wide = low.astype(F32)
                square_s[:, across] += wide * wide

            out(k).start()

        for k in range(-2, len(gs)):
            if k >= 2:
                out(k - 2).wait()
            if k + 2 < len(gs):
                start(k + 2)
            if k >= 0:
                finish(k)
        for k in range(max(len(gs) - 2, 0), len(gs)):
            out(k).wait()


    wqkv_s, wo_s = p1.at[:, pl.ds(0, three)], p1.at[:, pl.ds(three, d)]

    def transposed_dot(lhs, w, here):
        return _dot_turned(lhs[...], w[here, :])

    def hidden(first, many):
        def part(j, here):
            gate = _dot(b_s[...], p1[:, here])
            up = _dot(b_s[...], p2[:, here])
            by = transposed_dot(by_s, p3, here).astype(BF16).astype(F32)
            sig = jax.nn.sigmoid(gate)
            bu_s[:, here] = (by * (gate * sig)).astype(BF16)
            bg_s[:, here] = (by * up * (sig * (1 + gate * (1 - sig)))).astype(BF16)

        width = p1.shape[1]

        @pl.loop(first, min(first + many, width // TILE))
        def _(j):
            part(j, pl.ds(pl.multiple_of(j * TILE, TILE), TILE))

        if first + many > width // TILE and width % TILE:
            part(width // TILE, pl.ds(width // TILE * TILE, width % TILE))

    def project_back(w, src, dst):
        def part(j, here):
            dst[:, here] = transposed_dot(src, w, here).astype(BF16)

        _tiles(d, part)

    def by_b():
        def part(j, here):
            bb_s[:, here] = (transposed_dot(bg_s, p1, here) + transposed_dot(bu_s, p2, here)).astype(BF16)

        _tiles(d, part)


    def layer_steps(n):
        s = outs[n]
        grad = lambda kind: of[n, kind]

        def start():
            fetch("hid_t", s["hid_t"], p3)
            for name, dst in (("b", b_s), ("g", p1), ("u", p2), ("heads", qkv_s), ("lse", lse_s), ("hm", hm_s), ("att", o_s)):
                fetch(name, s[name], dst)

        def by_down():
            need("hid_t")
            _rows_out(p3, by_s, high_s, grad("d").whole, store, 0, ff // high_s.shape[1])
            fetch("d", s["d"], p3)

        def start_last():
            fetch("d", s["d"], p3)
            all_sent()
            for key in list(saving):
                kept(*key)

        def hidden_first():
            need("d")
            if n < top:
                need("b", "g", "u", "hm", "att", "heads", "lse")
            _flip(b_s, t_s)
            hidden(0, 4)

        def by_part(kind, src):
            g = grad(kind)
            _columns_out(t_s, src.at[:, g.across], wide_s, g.whole, store)

        def hidden_last():
            hidden(10, 3)
            fetch("a", s["a"], a_s)

        def by_mid():
            fetch("o", s["o"], wo_s)
            fetch("qkv", s["qkv"], wqkv_s)
            _norm_back(hm_s, bb_s, by_s)
            if n:
                fetch("h", outs[n - 1]["states"], hm_s)

        def by_o():
            _flip(o_s, t_s)
            _columns_out(t_s, by_s, wide_s, grad("o").whole, store)

        def by_att():
            need("o")
            project_back(wo_s, by_s, bb_s)

        def attention(iq):
            if iq == 0:
                dk_s[...] = jnp.zeros(dk_s.shape, F32)
                dv_s[...] = jnp.zeros(dv_s.shape, F32)
            _attend_rows_back(iq, qkv_s, o_s, bb_s, lse_s, bq_s, dq_s, dk_s, dv_s, cos_ref, sin_ref, HEAD**-0.5)

        def by_qkv():
            need("a", "qkv")
            _flip(a_s, t_s)
            _columns_out(t_s, bq_s, wide_s, grad("qkv").whole, store)

        def by_states():
            project_back(wqkv_s, bq_s, bb_s)
            need("h")
            _norm_back(hm_s, bb_s, by_s)

        f = functools.partial
        do = lambda what, *kinds: [f(what, grad(kind)) for kind in kinds]
        part = lambda kind: [f(by_part, kind, bg_s if kind[0] == "g" else bu_s)] + do(pair, kind)
        if n == top:
            steps = [start_last, hidden_first]
        else:
            steps = [start, by_down] + do(pair, "d") + [f(passed, of[n + 1, "qkv"]), hidden_first] + do(summed, "d") + [f(back, of[n + 1, "o"])]
        steps += [f(hidden, 4, 3)] + part("g0") + part("u0") + do(summed, "g0") + [f(hidden, 7, 3)] + do(summed, "u0") + [hidden_last]
        steps += do(passed, "d") + part("g1") + part("u1") + do(summed, "g1") + [by_b] + do(passed, "g0") + do(summed, "u1") + do(back, "d")
        steps += [by_mid, by_o] + do(pair, "o") + do(passed, "u0") + [by_att] + do(summed, "o") + do(back, "g0") + do(passed, "g1")
        steps += (do(late, "g0", "u0") if n == top else []) + do(back, "u0") + do(passed, "u1") + [f(attention, 0)] + do(back, "g1") + do(passed, "o")
        steps += (do(late, "g1", "u1") if n == top else []) + [f(attention, 1)] + do(back, "u1") + [by_qkv] + do(pair, "qkv")
        return steps + ([by_states] if n else []) + do(summed, "qkv") + (do(late, "o") if n == top else [])


    work = []
    f = functools.partial
    first = of[top, "d"]
    for n in range(layers):
        work += [((), 1.4, f(prepare, n)), ([(n, "qkv0"), (n, "qkv1")], 4, f(project, n, 0, 3)), ((), 2.4, f(project, n, 3, 3))]
        work.append(((), 4, f(attention_rows, n, 0, 1)))
        for iq in range(1, tokens // BQ):
            work += [((), 4, f(attention_rows, n, iq, 0)), ((), 4, f(attention_rows, n, iq, 1))]
        work += [([(n, "o")], 3, f(attended, n)), ((), 1.4, f(prepared, n))]
        for part in range(PARTS):
            tiles = held[f"g{part}"].shape[1] // LANES
            low = tiles // 2
            needs = [(n, f"g{part}"), (n, f"u{part}")]
            work += [(needs, low * 0.75 + 1, f(gated, n, part, 0, low)), ((), tiles * 0.75 / 2, f(gated, n, part, low, tiles - low))]
            if n == top:
                work.append(((), tiles * 0.35, f(last_down, part)))
                if part == PARTS - 2:
                    work.append(((), 0.1, f(pair, first, range(FAR))))
            else:
                work.append(((), tiles * 0.25, f(flipped, n, part)))
        if n < top:
            work += [([(n, f"d{part}")], 4.5, f(down, n, part * d // 512, d // 512)) for part in range(2)]
    rest = [((), 6, f(summed, first, "first")), ((), 0, f(late, first)), ((), 0, f(pair, first, [FAR]))]
    work[-1:] = [*rest[:2], work[-1], rest[2]]
    square_s[...] = jnp.zeros(square_s.shape, F32)
    for stage, what in _schedule(units, work):
        what() if stage == "run" else arrived(stage, what)
    steps = layer_steps(top)
    steps.insert(2, f(summed, first, "rest"))
    for n in reversed(range(top)):
        steps += layer_steps(n)
    for step in steps:
        step()
    end = grads[-1]
    waiting = [of[0, kind] for kind in GRADS[:5]] + [of[top, "qkv"], of[0, "o"], end]
    sent_far(of[0, "u1"])
    for g in waiting[:2]:
        late(g)
    back(of[top, "qkv"])
    passed(end)
    back(of[0, "o"])
    last([of[top, kind] for kind in GRADS[:6]])
    back(end)
    sent_far(end)

    for g, following in zip(waiting, waiting[2:]):
        pl.when(at_end)(lambda g=g: wait_block(g, send.at[g.number, LATE]))
        late(following)
    last(waiting)

    table_s[way] = jnp.full(table_s.shape[1:], jnp.sum(square_s[...]), F32)
    copies = []
    for j, device in enumerate(peers):
        copies.append(pltpu.make_async_remote_copy(src_ref=table_s.at[way], dst_ref=table_s.at[way], send_sem=meet.at[0, j],
                                                   recv_sem=meet.at[1, j], device_id=device, device_id_type=MESH))
        copies[-1].start()
    for copy in copies:
        copy.wait()
    total = table_s[0]
    for j in range(1, WAYS):
        total = total + table_s[j]
    squares[...] = total

    for g in grads:
        wait(g.at(g.swapped, 0, FAR), send.at[g.number, PAIR])
        wait_block(g, send.at[g.number, PAIR_LAST])
        sent_late = lambda g=g: wait_block(g, send.at[g.number, LATE])
        pl.when(inner)(sent_late) if g in waiting[:-2] else sent_late()
        far = lambda g=g: wait_block(g, send.at[g.number, FAR_ONE], send.at[g.number, FAR_TWO])
        pl.when(inner)(far) if g in (end, of[0, "u1"]) else far()


def turning(tokens):
    side = math.isqrt(tokens)
    turn = float(THETA) ** (-np.arange(HEAD // 2) / (HEAD // 2))
    tables = []
    for places in (np.arange(side), np.arange(tokens // side) * side):
        cos, sin = (np.concatenate([f(places[:, None] * turn)] * 2, 1) for f in (np.cos, np.sin))
        tables += [cos, sin, np.where(np.arange(HEAD) < HEAD // 2, -sin, sin)]
    return np.stack(tables).astype(np.float32)


def both_passes(x, dy, weights):
    wq, wk, wv, wo, wg, wu, wd = weights
    layers, (tokens, wide) = wq.shape[0], x.shape
    ff, kv, heads = wg.shape[2], wk.shape[2], wide // HEAD
    three = wide + 2 * kv
    big = lambda *shape: jax.ShapeDtypeStruct(shape, BF16)
    whole = dict(qkv=big(wide, three), o=big(wide, wide), g=big(wide, ff), u=big(wide, ff), d=big(ff, wide))
    square = big(tokens, wide)
    saved = dict(a=square, heads=big(tokens, three), att=square, lse=jax.ShapeDtypeStruct((heads, tokens), F32), hm=square, b=square,
                 states=square, hid_t=big(ff, tokens))
    outs = [*whole.values(), *(saved[name] for name in SAVED)] * layers
    where = {}
    for n in reversed(range(layers)):
        for kind in GRAD_ARRAYS:
            rows, columns = whole[kind].shape
            part = rows // WAYS
            outs += [whole[kind], *[big(rows // 2, columns)] * 2, big(part * (CAME - FROM_END), columns), big(part, columns)]
            where[n, kind] = len(outs) - 1
    vm = lambda *shape: pltpu.VMEM(shape, BF16)
    f32 = lambda *shape: pltpu.VMEM(shape, F32)
    sems = lambda *shape: pltpu.SemaphoreType.DMA(shape)
    units, count = layers * len(KINDS), layers * len(GRADS)
    got = pl.pallas_call(
        functools.partial(_both_passes, layers),
        in_specs=[EVERY] * 9 + [INNER],
        out_specs=[EVERY] * len(outs) + [INNER],
        out_shape=[*outs, jax.ShapeDtypeStruct((8, LANES), F32)],
        scratch_shapes=[vm(wide, ff), vm(wide, ff), vm(ff, wide), vm(tokens, ff), vm(tokens, ff), *[vm(tokens, wide)] * 6, vm(tokens, three),
                        vm(tokens, three), f32(heads, HEAD + 8, BQ), *[f32(kv // HEAD, tokens, HEAD)] * 2, f32(heads, BQ), f32(heads, tokens),
                        vm(2, wide, TILE), vm(2, ff // 10, wide), f32(PACK, ff), f32(WAYS, 8, LANES), f32(tokens, HEAD), f32(tokens, HEAD),
                        sems(units, OWN + 1), sems(units, OWN + 1), sems(units, 2), sems(layers, len(WHOLE)), sems(layers, len(SAVED)),
                        sems(count, PAIR_LAST + 1), sems(count, CAME + 1), sems(len(FETCHED)), sems(2), sems(2, WAYS - 1)],
        compiler_params=pltpu.CompilerParams(collective_id=0, has_side_effects=True, vmem_limit_bytes=67043328),
        cost_estimate=pl.CostEstimate(flops=270 * 10**9, bytes_accessed=6 * 10**8, transcendentals=10**7),
        name="both_passes",
    )(x, dy, *weights, turning(tokens))
    return [{kind: got[where[n, kind]] for kind in GRAD_ARRAYS} for n in range(layers)], got[-1]


def _step(layers, count, squares, *refs):
    kinds = len(NAMES)
    w, m, v = refs[:kinds], refs[kinds : 2 * kinds], refs[2 * kinds : 3 * kinds]
    refs = refs[3 * kinds :]
    grads, refs = [dict(zip(GRAD_ARRAYS, refs[n * len(GRAD_ARRAYS) :])) for n in range(layers)], refs[layers * len(GRAD_ARRAYS) :]
    outs, refs = refs[: 3 * kinds], refs[3 * kinds :]
    held, g_held, came, g_came, left = refs[: 3 * kinds], dict(zip(GRAD_ARRAYS, refs[3 * kinds :])), *refs[-3:]
    reads, of = {}, dict(zip(NAMES, [("qkv", 0), ("qkv", w[0].shape[2]), ("qkv", w[0].shape[2] + w[1].shape[2]), ("o", 0), ("g", 0), ("u", 0), ("d", 0)]))
    for n in range(layers):
        for i, kind in enumerate(GRAD_ARRAYS):
            reads[n, kind] = pltpu.make_async_copy(grads[n][kind], g_held[kind].at[n], g_came.at[n, i])
            reads[n, kind].start()
        for i in range(kinds):
            for x, src in enumerate((w[i], m[i], v[i])):
                reads[n, i, x] = pltpu.make_async_copy(src.at[n], held[x * kinds + i].at[n], came.at[n, i, x])
                reads[n, i, x].start()
    factor = jnp.minimum(1.0, 0.5 * lax.rsqrt(squares[...] / count + 1e-30))[:1, :1]
    writes = []
    for n in range(layers):
        for i, name in enumerate(NAMES):
            kind, first = of[name]
            if (n, kind) in reads:
                reads.pop((n, kind)).wait()
            for x in range(3):
                reads[n, i, x].wait()
            w_s, m_s, v_s = (held[x * kinds + i].at[n] for x in range(3))
            g_s = g_held[kind].at[n, :, pl.ds(first, w_s.shape[1])]

            @pl.loop(0, w_s.shape[0] // PACK)
            def _(j):
                rows = pl.ds(pl.multiple_of(j * PACK, PACK), PACK)
                g, old = g_s[rows, :].astype(F32) * factor, w_s[rows, :].astype(F32)
                new_m = 0.9 * m_s[rows, :] + 0.1 * g
                new_v = 0.95 * v_s[rows, :] + 0.05 * g * g
                m_s[rows, :] = new_m
                v_s[rows, :] = new_v
                w_s[rows, :] = (old - 0.02 * (new_m * lax.rsqrt(new_v + 1e-8) + 0.1 * old)).astype(BF16)

            for x, src in enumerate((w_s, m_s, v_s)):
                writes.append(pltpu.make_async_copy(src, outs[x * kinds + i].at[n], left.at[n, i, x]))
                writes[-1].start()
    for copy in writes:
        copy.wait()


def take_step(squares, weights, m, v, parts):
    layers, kinds = weights[0].shape[0], len(weights)
    sems = lambda *shape: pltpu.SemaphoreType.DMA(shape)
    like = [jax.ShapeDtypeStruct(t.shape, t.dtype) for t in (*weights, *m, *v)]
    return pl.pallas_call(
        functools.partial(_step, layers, WAYS * sum(t.size for t in weights)),
        in_specs=[INNER] + [EVERY] * (3 * kinds + layers * len(GRAD_ARRAYS)),
        out_specs=[EVERY] * len(like),
        out_shape=like,
        scratch_shapes=[pltpu.VMEM(t.shape, t.dtype) for t in like] + [pltpu.VMEM((layers, *parts[0][kind].shape), BF16) for kind in GRAD_ARRAYS]
        + [sems(layers, kinds, 3), sems(layers, len(GRAD_ARRAYS)), sems(layers, kinds, 3)],
        compiler_params=pltpu.CompilerParams(vmem_limit_bytes=67043328),
        name="take_step",
    )(squares, *weights, *m, *v, *[part[kind] for part in parts for kind in GRAD_ARRAYS])


def solution(mesh):
    def step(x, dy, *arrays):
        weights, m, v = (arrays[i : i + len(NAMES)] for i in range(0, len(arrays), len(NAMES)))
        parts, squares = both_passes(x[0], dy[0], weights)
        return tuple(take_step(squares, weights, m, v, parts))

    states, cut = P(("rep", "dp"), None, None), P(None, "dp", None)
    return jax.shard_map(
        step,
        mesh=mesh,
        in_specs=(states, states) + (cut,) * 21,
        out_specs=(P("rep", "dp", None),) * 21,
        check_vma=False,
    )
```

```python
import functools
import math

import jax
import jax.numpy as jnp
import numpy as np
from jax import lax
from jax.experimental import pallas as pl
from jax.experimental.pallas import tpu as pltpu
from jax.sharding import PartitionSpec as P

NEG = -1e30
HIDDEN = 2 * NEG
LOG2E = 1.4426950408889634


def _dot(a, b):
    return jnp.dot(a, b, preferred_element_type=jnp.float32)


def _dot_turned(a, b):
    return lax.dot_general(a, b, (((1,), (1,)), ((), ())), preferred_element_type=jnp.float32)


HEAD = 128
THETA = 10000
F32, BF16 = jnp.float32, jnp.bfloat16
MESH = pl.DeviceIdType.MESH
REPS, WAYS, LINE = 4, 8, 4
TILE, LANES, PACK = 256, 128, 16
BQ, BK = 512, 256
TO_Z, TO_X, TO_Y, ON, SWAP, OWN = range(6)
FAR = LINE - 1
ENDS, INNERS = (0, LINE - 1), range(1, LINE - 1)
START, PACE, BEFORE = 24.0, 3.0, dict(Z=24, P=14, F=6, S=0)
SHIFT = {("S", "q"): -3, ("F", "o"): 3}
AHEAD = 2
KINDS = ("qkv0", "qkv1", "o", "g0", "u0", "g1", "u1", "g2", "u2", "d0", "d1")
PARTS = 3
NAMES = ["wq", "wk", "wv", "wo", "w_gate", "w_up", "w_down"]
WHOLE = ["qkv", "o", "g", "u", "d"]
SAVED = ["a", "heads", "att", "lse", "hm", "b", "states", "hid_t"]
GRADS = ["d", "g0", "u0", "g1", "u1", "o", "qkv"]
GRAD_ARRAYS = ["d", "g", "u", "o", "qkv"]
FETCHED = ["by", "hid_t", "b", "d", "g", "u", "hm", "att", "a", "heads", "lse", "o", "qkv", "h"]
AT_ONCE = 4
PAIR, FAR_ONE, FAR_TWO, LATE, PAIR_LAST = range(5)
FROM_END, FROM_MID, CAME = 1, 4, 6
EVERY = pl.BlockSpec(memory_space=pl.ANY)
INNER = pl.BlockSpec(memory_space=pltpu.VMEM)


class Unit:
    def __init__(self, number, layer, kind, block, whole, held, first):
        self.number, self.layer, self.kind, self.block, self.whole, self.held = number, layer, kind, block, whole, held
        self.first, self.width, self.rows = first, held.shape[1], whole.shape[0] // WAYS
        self.by_columns = self.rows // REPS % PACK != 0

    def cut(self, ref, base, place):
        part = (self.width if self.by_columns else self.rows) // REPS
        if place is None:
            return ref.at[pl.ds(pl.multiple_of(base, 8), self.rows), pl.ds(self.first, self.width)]
        if self.by_columns:
            return ref.at[pl.ds(pl.multiple_of(base, 8), self.rows), pl.ds(pl.multiple_of(self.first + place * part, LANES), part)]
        return ref.at[pl.ds(pl.multiple_of(base + place * part, part), part), pl.ds(self.first, self.width)]

    def own(self, place=None):
        return self.cut(self.block, 0, place)

    def part(self, way, place=None):
        return self.cut(self.whole, way * self.rows, place)

    def bytes_of(self, quarters):
        if self.by_columns:
            return self.whole.at[pl.ds(0, -(-quarters // REPS) * self.rows), pl.ds(self.first, min(quarters, REPS) * self.width // REPS)]
        return self.whole.at[pl.ds(0, quarters * self.rows // REPS), pl.ds(self.first, self.width)]


def _norm(src, dst, rows=LANES):
    @pl.loop(0, src.shape[0] // rows)
    def _(i):
        here = pl.ds(pl.multiple_of(i * rows, rows), rows)
        wide = src[here, :].astype(F32)
        scale = lax.rsqrt(jnp.mean(wide * wide, -1, keepdims=True) + 1e-6)
        dst[here, :] = (wide * scale).astype(BF16)


def _columns(lhs, w, tiles, width, use, first=0):
    @pl.loop(first, first + tiles)
    def _(j):
        here = pl.ds(pl.multiple_of(j * width, width), width)
        use(j, here, _dot(lhs[...], w[:, here]))


def _head(n):
    return slice(n * HEAD, (n + 1) * HEAD)


def _attend_rows(iq, part, qkv_s, o_s, lse_s, top_s, mix_s, scale):
    heads, d = top_s.shape[0], HEAD
    group = 2 * heads // (qkv_s.shape[1] // HEAD - heads)
    e = scale * LOG2E
    rows = pl.ds(iq * BQ, BQ)
    whole = iq * BQ // BK
    if part == 0 or not whole:
        top_s[...] = jnp.full(top_s.shape, NEG, F32)
        mix_s[...] = jnp.zeros(mix_s.shape, F32)
    ones = jnp.ones((8, BK), BF16)

    def block(j, masked):
        here = pl.ds(pl.multiple_of(j * BK, BK), BK)
        scores = [_dot_turned(qkv_s[here, _head(heads + n // group)], qkv_s[rows, _head(n)]) for n in range(heads)]
        if masked:
            gap = lax.broadcasted_iota(jnp.int32, (BK, BQ), 1) - lax.broadcasted_iota(jnp.int32, (BK, BQ), 0)
            ok = gap >= j * BK - iq * BQ
        weights, keeps = [], []
        for n, s in enumerate(scores):
            if masked:
                s = jnp.where(ok, s, HIDDEN)
            old = top_s[n : n + 1, :]
            top = jnp.maximum(old, s.max(axis=0, keepdims=True))
            top_s[n : n + 1, :] = top
            weights.append(jnp.exp2((s - top) * e).astype(BF16))
            keeps.append(jnp.exp2((old - top) * e))
        for n, (p, keep) in enumerate(zip(weights, keeps)):
            values = jnp.concatenate([qkv_s[here, _head(heads + (heads + n) // group)].T, ones], axis=0)
            mix_s[n] = mix_s[n] * keep + _dot(values, p)

    if part == 0:
        lax.fori_loop(0, whole, lambda j, _: block(j, False), None)
        return
    lax.fori_loop(whole, whole + BQ // BK, lambda j, _: block(j, True), None)
    for n in range(heads):
        total = mix_s[n, d : d + 1, :]
        o_s[rows, _head(n)] = (mix_s[n, :d, :] * (1 / total)).T.astype(BF16)
        lse_s[n : n + 1, rows] = top_s[n : n + 1, :] * scale + jnp.log(total)


def _flip(src, dst):
    @pl.loop(0, src.shape[0] // LANES)
    def _(i):
        here = pl.ds(pl.multiple_of(i * LANES, LANES), LANES)
        dst[:, here] = src[here, :].T


def _flip_out(src, out_s, dst, sems, first, width):
    def copy(i, slot):
        return pltpu.make_async_copy(out_s.at[slot, pl.ds(0, LANES), :], dst.at[pl.ds(pl.multiple_of(i * LANES, LANES), LANES), :], sems.at[slot])

    start, end = first // LANES, (first + width) // LANES

    @pl.loop(start, end)
    def _(i):
        slot = lax.rem(i, 2)

        @pl.when(i >= start + 2)
        def _():
            copy(i - 2, slot).wait()

        out_s[slot, :LANES, :] = src[:, pl.ds(pl.multiple_of(i * LANES, LANES), LANES)].T
        copy(i, slot).start()

    for i in (end - 2, end - 1):
        copy(i, i % 2).wait()


def _rows_out(lhs, rhs, out_s, dst, sems, first, total, high):
    steps = total // high

    def rows(i):
        return pl.ds(pl.multiple_of(first + i * high, PACK), high)

    def copy(i, slot):
        return pltpu.make_async_copy(out_s.at[slot, pl.ds(0, high), :], dst.at[rows(i), :], sems.at[slot])

    @pl.loop(0, steps)
    def _(i):
        slot = lax.rem(i, 2)

        @pl.when(i >= 2)
        def _():
            copy(i - 2, slot).wait()

        out_s[slot, :high, :] = _dot(lhs[rows(i), :], rhs[...]).astype(BF16)
        copy(i, slot).start()

    for i in (steps - 2, steps - 1):
        copy(i, i % 2).wait()


class Gradient:
    def __init__(self, number, layer, kind, refs, first, columns):
        self.number, self.layer, self.kind, self.first, self.columns = number, layer, kind, first, columns
        whole, self.swapped, self.sums, self.came, out = refs
        self.rows = out.shape[0]
        across = pl.ds(first, columns)
        self.whole, self.out = whole.at[:, across], out.at[:, across]
        self.across = across

    def at(self, ref, block, many=1):
        return ref.at[pl.ds(pl.multiple_of(block * self.rows, 8), many * self.rows), self.across]

    def own(self, block):
        return self.whole.at[pl.ds(pl.multiple_of(block * self.rows, 8), self.rows), :]


def _tiles(width, use, size=TILE):
    @pl.loop(0, width // size)
    def _(j):
        use(j, pl.ds(pl.multiple_of(j * size, size), size))

    if width % size:
        use(width // size, pl.ds(width // size * size, width % size))


def _columns_out(lhs, rhs, out_s, dst, sems):
    width = rhs.shape[1]
    steps = -(-width // TILE)

    def copy(j, here, slot):
        return pltpu.make_async_copy(out_s.at[slot, :, pl.ds(0, here.size)], dst.at[:, here], sems.at[slot])

    def part(j, here):
        slot = lax.rem(j, 2) if not isinstance(j, int) else j % 2
        before = pl.ds(pl.multiple_of((j - 2) * TILE, TILE), TILE)
        if isinstance(j, int):
            copy(j - 2, before, slot).wait()
        else:
            pl.when(j >= 2)(lambda: copy(j - 2, before, slot).wait())
        out_s[slot, :, : here.size] = _dot(lhs[...], rhs[:, here]).astype(BF16)
        copy(j, here, slot).start()

    _tiles(width, part)
    for j in (steps - 2, steps - 1):
        copy(j, pl.ds(j * TILE, min(TILE, width - j * TILE)), j % 2).wait()


def _norm_back(h, by_normed, by, first=False, rows=LANES):
    @pl.loop(0, by.shape[0] // rows)
    def _(i):
        here = pl.ds(pl.multiple_of(i * rows, rows), rows)
        wide, grad = h[here, :].astype(F32), by_normed[here, :].astype(F32)
        scale = lax.rsqrt(jnp.mean(wide * wide, -1, keepdims=True) + 1e-6)
        along = jnp.mean(wide * grad, -1, keepdims=True)
        by[here, :] = by[here, :] + (scale * grad - wide * (scale * scale * scale * along)).astype(BF16)


def _attend_rows_back(iq, qkv_s, att_s, by_att_s, lse_s, by_s, dq_s, dk_s, dv_s, cos_ref, sin_ref, scale):
    heads, d = lse_s.shape[0], HEAD
    group = 2 * heads // (qkv_s.shape[1] // HEAD - heads)
    e = scale * LOG2E
    rows = pl.ds(iq * BQ, BQ)
    dq_s[...] = jnp.zeros(dq_s.shape, F32)
    rotated = lambda t, c, s: (t * c - pltpu.roll(t, HEAD // 2, 1) * s).astype(BF16)

    for i in range(heads // group):
        mine = range(i * group, (i + 1) * group)
        lses = [lse_s[n : n + 1, rows] * LOG2E for n in mine]
        deltas = [(by_att_s[rows, _head(n)].astype(F32) * att_s[rows, _head(n)].astype(F32)).T.sum(axis=0, keepdims=True) for n in mine]

        def block(j, masked):
            here = pl.ds(pl.multiple_of(j * BK, BK), BK)
            k, v = qkv_s[here, _head(heads + i)], qkv_s[here, _head(heads + heads // group + i)]
            if masked:
                gap = lax.broadcasted_iota(jnp.int32, (BK, BQ), 1) - lax.broadcasted_iota(jnp.int32, (BK, BQ), 0)
                ok = gap >= j * BK - iq * BQ
            qs, dos = [qkv_s[rows, _head(n)] for n in mine], [by_att_s[rows, _head(n)] for n in mine]
            scores, dps = [_dot_turned(k, q) for q in qs], [_dot_turned(v, t) for t in dos]
            for x, n in enumerate(mine):
                p = jnp.exp2(scores[x] * e - lses[x])
                if masked:
                    p = jnp.where(ok, p, 0.0)
                ds = (p * (dps[x] - deltas[x])).astype(BF16)
                dv_s[i, here, :] += _dot(p.astype(BF16), dos[x])
                dk_s[i, here, :] += _dot(ds, qs[x])
                dq_s[n] += _dot(k.T, ds)

        whole = iq * BQ // BK
        if whole:
            lax.fori_loop(0, whole, lambda j, _: block(j, False), None)
        lax.fori_loop(whole, whole + BQ // BK, lambda j, _: block(j, True), None)
        for n in mine:
            dq = (dq_s[n] * scale).T.astype(BF16).astype(F32)
            by_s[rows, _head(n)] = rotated(dq, cos_ref[rows, :], sin_ref[rows, :])

    if (iq + 1) * BQ == qkv_s.shape[0]:
        for i in range(heads // group):
            dk = (dk_s[i] * scale).astype(BF16).astype(F32)
            by_s[:, _head(heads + i)] = rotated(dk, cos_ref[...], sin_ref[...])
            by_s[:, _head(heads + heads // group + i)] = dv_s[i].astype(BF16)


def p_half(ff):
    return (ff // TILE + 1) // 2 * TILE + TILE


def _schedule(units, work):
    came, when, ready = 0.0, [], {}
    for u in units:
        came += u.whole.shape[0] * u.width * 2e-6
        done = START + came * PACE
        for stage, before in BEFORE.items():
            shift = SHIFT.get((stage, u.kind[0]), 0) * (u.layer > 0)
            when.append((done - before * (1 + came / 100) + shift, stage, u))
        ready[u.layer, u.kind] = done
    when.sort(key=lambda e: e[0])
    order, now, work = [], 0.0, list(work)
    while when or work:
        able = work and all(ready[n] <= now for n in work[0][0]) and not [e for e in when if e[1] == "S" and (e[2].layer, e[2].kind) in work[0][0]]
        if when and (when[0][0] <= now or not able):
            order.append(when[0][1:])
            now = max(now, when.pop(0)[0])
        else:
            order.append(("run", work[0][2]))
            now += work.pop(0)[1]
    return order


def _both_passes(layers, x_ref, dy_ref, wq_b, wk_b, wv_b, o_b, g_b, u_b, d_b, turns_ref, *refs):
    each = len(WHOLE) + len(SAVED)
    outs = [dict(zip(WHOLE + SAVED, refs[n * each : n * each + each])) for n in range(layers)]
    refs = refs[layers * each :]
    grads = []
    half = p_half(outs[0]["g"].shape[1])
    for n in reversed(range(layers)):
        for name in GRAD_ARRAYS:
            five, refs = refs[:5], refs[5:]
            wide = five[0].shape[1]
            for part, first, columns in [("0", 0, half), ("1", half, wide - half)] if name in ("g", "u") else [("", 0, wide)]:
                grads.append(Gradient(len(grads), n, name + part, five, first, columns))
    grads.sort(key=lambda g: (-g.layer, GRADS.index(g.kind)))
    of = {(g.layer, g.kind): g for g in grads}
    (squares, p1, p2, p3, bg_s, bu_s, by_s, a_s, o_s, hm_s, bb_s, t_s, qkv_s, bq_s, mix_s, dk_s, dv_s, top_s, lse_s, wide_s, high_s,
     square_s, table_s, cos_ref, sin_ref, w_send, w_recv, load, stage_in, save, send, recv, fetching, store, meet) = refs
    tokens, d = by_s.shape
    heads, ff, three = lse_s.shape[0], p1.shape[1], qkv_s.shape[1]
    top = layers - 1
    side = -(-ff // LINE // LANES) * LANES
    spans = [(0, side), (ff - side, side), (side, ff - 2 * side)]
    hid_s, b_s, dq_s = bg_s, a_s, mix_s.at[:, pl.ds(0, HEAD), :]

    rep, way = lax.axis_index("rep"), lax.axis_index("dp")
    core, z = lax.rem(way, 2), lax.div(way, 2)
    px, py = lax.div(rep, 2), lax.rem(rep, 2)
    by_x, by_y = (1 - px) * 2 + py, px * 2 + 1 - py
    other = (rep, z * 2 + 1 - core)
    far_ways = [lax.rem(z + j, LINE) * 2 + core for j in range(1, LINE)]
    third = by_y * (1 - core) + by_x * core, by_x * (1 - core) + by_y * core
    at_end = (z == 0) | (z == LINE - 1)
    inner = jnp.logical_not(at_end)
    on = jnp.where((z == 0) | (z == 1), 1, -1)
    chip = lambda to: (rep, to * 2 + core)
    peers = [(rep, lax.rem(way + j, WAYS)) for j in range(1, WAYS)]

    widths = dict(qkv=three // 2, d=d // 2)
    held = dict(qkv0=bq_s.at[:, pl.ds(0, three // 2)], qkv1=bq_s.at[:, pl.ds(three // 2, three // 2)], o=bb_s, d0=p3.at[:, pl.ds(0, d // 2)], d1=p3.at[:, pl.ds(d // 2, d // 2)])
    for part in range(PARTS):
        across = pl.ds(*spans[part])
        held[f"g{part}"], held[f"u{part}"] = p1.at[:, across], p2.at[:, across]
    units, staged = [], {}
    rows = g_b.shape[1]
    for n in range(layers):
        strip = lambda i, first, wide: bu_s.at[pl.ds(i * rows, rows), pl.ds(first, wide)]
        places = dict(g=strip(n, 0, ff), u=strip(layers + n, 0, ff), qkv=strip(2 * layers, n * three, three), o=strip(2 * layers + 1, n * d, d),
                      d=t_s.at[pl.ds(n * d_b.shape[1], d_b.shape[1]), :])
        parts = dict(g=[g_b], u=[u_b], qkv=[wq_b, wk_b, wv_b], o=[o_b], d=[d_b])
        for i, name in enumerate(WHOLE):
            at = 0
            for src in parts[name]:
                to_place = places[name].at[:, pl.ds(at, src.shape[2])]
                pltpu.make_async_copy(src.at[n], to_place, stage_in.at[n, i]).start()
                at += src.shape[2]
            staged[n, name] = pltpu.make_async_copy(places[name], places[name], stage_in.at[n, i])
        for kind in KINDS:
            name, part = kind.rstrip("012"), kind[-1]
            first = (spans[int(part)][0] if name in "gu" else int(part) * widths[name]) if part.isdigit() else 0
            units.append(Unit(len(units), n, kind, places[name], outs[n][name], held[kind], first))

    coming, saving = {}, {}

    def fetch(name, src, dst):
        copy = pltpu.make_async_copy(src, dst, fetching.at[FETCHED.index(name)])
        copy.start()
        coming[name] = copy

    def need(*what):
        for name in what:
            coming.pop(name).wait()

    def keep(n, name, src, dst):
        if n < top or name == "a":
            copy = pltpu.make_async_copy(src, dst, save.at[n, SAVED.index(name)])
            copy.start()
            saving[n, name] = copy

    def kept(n, *what):
        for name in what:
            if (n, name) in saving:
                saving.pop((n, name)).wait()

    def wait(ref, sem):
        pltpu.make_async_copy(ref, ref, sem).wait()

    fetch("h", x_ref, by_s)

    @pl.loop(0, tokens // turns_ref.shape[1])
    def _(i):
        near_cos, near_sin, near_signed = (turns_ref[x] for x in range(3))
        far_cos, far_sin, far_signed = (turns_ref[3 + x, pl.ds(i, 1), :] for x in range(3))
        here = pl.ds(pl.multiple_of(i * turns_ref.shape[1], 8), turns_ref.shape[1])
        cos_ref[here, :] = far_cos * near_cos - far_sin * near_sin
        sin_ref[here, :] = far_signed * near_cos + far_cos * near_signed

    barrier = pltpu.get_barrier_semaphore()
    near = [(by_x, way), (by_y, way), *peers]
    for device in near:
        pl.semaphore_signal(barrier, inc=1, device_id=device, device_id_type=MESH)
    pl.semaphore_wait(barrier, len(near))


    def to(u, stage, src, dst, device):
        pltpu.make_async_remote_copy(src_ref=src, dst_ref=dst, send_sem=w_send.at[u.number, stage], recv_sem=w_recv.at[u.number, stage],
                                     device_id=device, device_id_type=MESH).start()

    def wait_for(u, quarters, *sems):
        for sem in sems:
            wait(u.bytes_of(quarters), sem)

    def begin(u):
        place = u.layer, u.kind.rstrip("012")
        if place in staged:
            staged.pop(place).wait()
        for w in far_ways:
            to(u, TO_Z, u.own(rep), u.part(way, rep), (rep, w))
        to(u, OWN, u.own(), u.part(way), other)
        pltpu.make_async_copy(u.own(), u.part(way), load.at[u.number, 1]).start()

    for u in units[:AHEAD]:
        begin(u)

    def arrived(stage, u):
        came, at_home = w_recv.at[u.number], load.at[u.number]
        if stage == "Z":
            wait_for(u, FAR, came.at[TO_Z])
            if u.number + AHEAD < len(units):
                begin(units[u.number + AHEAD])
            for w in far_ways:
                to(u, TO_X, u.part(w, rep), u.part(w, rep), (by_x, way))
                to(u, TO_Y, u.part(w, rep), u.part(w, rep), (by_y, way))
        elif stage == "P":
            wait_for(u, FAR, came.at[TO_X], came.at[TO_Y])
            for w, (place, there) in zip(far_ways, ((by_y, by_x), (by_x, by_y), third)):
                to(u, ON, u.part(w, place), u.part(w, place), (there, way))
        elif stage == "F":
            wait_for(u, FAR, came.at[ON])
            for w in far_ways:
                to(u, SWAP, u.part(w), u.part(w), other)
        else:
            wait_for(u, FAR * REPS, came.at[SWAP])
            wait_for(u, REPS, came.at[OWN], at_home.at[1])
            if u.layer < top or u.kind[0] != "d":
                pltpu.make_async_copy(u.whole.at[:, pl.ds(u.first, u.width)], u.held, at_home.at[0]).start()

    def at_hand(n, *kinds):
        for kind in kinds:
            u = units[n * len(KINDS) + KINDS.index(kind)]
            pltpu.make_async_copy(u.whole.at[:, pl.ds(u.first, u.width)], u.held, load.at[u.number, 0]).wait()

    def all_sent():
        for u in units:
            sent = w_send.at[u.number]
            wait_for(u, FAR, *(sent.at[stage] for stage in (TO_Z, TO_X, TO_Y, ON)))
            wait_for(u, FAR * REPS, sent.at[SWAP])
            wait_for(u, REPS, sent.at[OWN])


    def prepare(n):
        kept(n - 1, "b", "heads")
        if n == 0:
            need("h")
        else:
            kept(n - 1, "hid_t")
        _norm(by_s, a_s)
        keep(n, "a", a_s, outs[n]["a"])

    def project(n, first, tiles):
        if first == 0:
            at_hand(n, "qkv0", "qkv1")

        def turn(j, here, acc):
            cos, sin = cos_ref[...], sin_ref[...]
            for half in range(2):
                t = acc[:, _head(half)].astype(BF16).astype(F32)
                t = (t * cos + pltpu.roll(t, HEAD // 2, 1) * sin).astype(BF16)
                qkv_s[:, pl.ds(pl.multiple_of((2 * j + half) * HEAD, HEAD), HEAD)] = t

        def value(j, here, acc):
            qkv_s[:, here] = acc.astype(BF16)

        turned = (three + d) // 512
        _columns(a_s, bq_s, min(tiles, turned - first), TILE, turn, first)
        if first + tiles > turned:
            _columns(a_s, bq_s, first + tiles - turned, TILE, value, turned)
            keep(n, "heads", qkv_s, outs[n]["heads"])

    def attention_rows(n, iq, part):
        if iq == 0:
            kept(n - 1, "att", "lse")
        _attend_rows(iq, part, qkv_s, o_s, lse_s, top_s, mix_s, HEAD**-0.5)
        if part and (iq + 1) * BQ == tokens:
            keep(n, "att", o_s, outs[n]["att"])
            keep(n, "lse", lse_s, outs[n]["lse"])

    def attended(n):
        kept(n - 1, "hm", "states")
        at_hand(n, "o")

        def add(j, here, acc):
            hm_s[:, here] = by_s[:, here] + acc.astype(BF16)

        _columns(o_s, bb_s, d // TILE, TILE, add)

    def prepared(n):
        keep(n, "hm", hm_s, outs[n]["hm"])
        kept(n, "a")
        _norm(hm_s, a_s)
        keep(n, "b", a_s, outs[n]["b"])
        if n == top:
            fetch("by", dy_ref, by_s)

    def gated(n, part, first, tiles):
        kinds = f"g{part}", f"u{part}"
        if first == 0:
            at_hand(n, *kinds)
        w_g, w_u = (held[kind] for kind in kinds)

        @pl.loop(first, first + tiles)
        def _(j):
            here = pl.ds(pl.multiple_of(j * LANES, LANES), LANES)
            acc = _dot(a_s[...], jnp.concatenate([w_g[:, here], w_u[:, here]], 1))
            gate, up = acc[:, :LANES], acc[:, LANES:]
            hidden = (jax.nn.silu(gate) * up).astype(BF16)
            across = pl.ds(pl.multiple_of(spans[part][0] + j * LANES, LANES), LANES)
            if n == top:
                p3[across, :] = hidden.T
            else:
                hid_s[:, across] = hidden

    def down(n, first, tiles):
        at_hand(n, "d1" if first else "d0")

        def add(j, here, acc):
            by_s[:, here] = hm_s[:, here] + acc.astype(BF16)

        _columns(hid_s, p3, tiles, TILE, add, first)
        if first:
            keep(n, "states", by_s, outs[n]["states"])

    def flipped(n, part):
        _flip_out(hid_s, high_s, outs[n]["hid_t"], store, *spans[part])

    def last_down(part):
        if part == 0:
            need("by")
        first, width = spans[part]
        _rows_out(p3, by_s, high_s, of[top, "d"].whole, store, first, width, width // 4)


    def remote(g, src, dst, sent, came, device):
        return pltpu.make_async_remote_copy(src_ref=src, dst_ref=dst, send_sem=send.at[g.number, sent], recv_sem=recv.at[g.number, came],
                                            device_id=device, device_id_type=MESH)

    def wait_block(g, *sems):
        for sem in sems:
            wait(g.at(g.came, 0), sem)

    def pair(g, blocks=range(LINE)):
        for there in blocks:
            sent, came = (PAIR, PAIR) if there in ENDS else (PAIR_LAST, CAME)
            remote(g, g.own(there * 2 + 1 - core), g.at(g.swapped, there), sent, came, other).start()

    def added(g, jobs, after=None):
        def scoped(buf, sems):
            loads, stores, at = [], [], 0
            for parts, _ in jobs:
                mine = []
                for ref in parts:
                    mine.append(pltpu.make_async_copy(ref, buf.at[at], sems.at[at]))
                    mine[-1].start()
                    at += 1
                loads.append((mine, at - len(parts)))
            for (mine, first), (parts, to) in zip(loads, jobs):
                for c in mine:
                    c.wait()

                @pl.loop(0, g.rows // PACK)
                def _(i):
                    here = pl.ds(pl.multiple_of(i * PACK, PACK), PACK)
                    total = buf[first, here, :].astype(F32)
                    for x in range(1, len(parts)):
                        total = total + buf[first + x, here, :].astype(F32)
                    low = total.astype(BF16)
                    buf[first, here, :] = low

                stores.append(pltpu.make_async_copy(buf.at[first], to, sems.at[first]))
                stores[-1].start()
            for x, c in enumerate(stores):
                c.wait()
                if after:
                    after(x)

        many = sum(len(parts) for parts, _ in jobs)
        pl.run_scoped(scoped, pltpu.VMEM((many, g.rows, g.columns), BF16), pltpu.SemaphoreType.DMA((many,)))

    def step_on(many):
        return jnp.clip(z + many * on, 0, LINE - 1)

    def terms(g, block):
        return [g.own(block * 2 + core), g.at(g.swapped, block)]

    def send_sum(g, block, sent, came, to):
        remote(g, g.at(g.sums, block), g.at(g.came, came - FROM_END), sent, came, chip(to)).start()

    def summed(g, *some):
        far, mid, near = step_on(3), step_on(2), step_on(1)
        job = lambda block: (terms(g, block), g.at(g.sums, block))
        send = (lambda _: send_sum(g, far, FAR_ONE, FROM_END, near)), (lambda _: send_sum(g, mid, FAR_TWO, FROM_END + 1, near))
        first, rest = "first" in some or not some, "rest" in some or not some
        if first:
            wait(g.at(g.swapped, 0, 2), recv.at[g.number, PAIR])
        if rest:
            wait(g.at(g.swapped, 0, 2), recv.at[g.number, CAME])

        @pl.when(at_end)
        def _():
            if not some:
                added(g, [job(far), job(mid)], lambda x: send[x](x))
                added(g, [job(near)])
            elif first:
                added(g, [job(far)], send[0])
            else:
                added(g, [job(mid), job(near)], lambda x: x or send[1](x))

    def late(g):
        pl.when(at_end)(lambda: send_sum(g, step_on(1), LATE, FROM_END + 2, step_on(1)))

    def sent_far(g):
        pl.when(at_end)(lambda: wait_block(g, send.at[g.number, FAR_ONE], send.at[g.number, FAR_ONE + 1]))

    def passed(g):
        far, mid = step_on(2), step_on(1)

        def jobs():
            for x, block in enumerate((far, mid)):
                wait_block(g, recv.at[g.number, FROM_END + x])
                added(g, [(terms(g, block) + [g.at(g.came, x)], g.at(g.sums, block))],
                      lambda _, x=x, block=block: send_sum(g, block, FAR_ONE + x, FROM_MID + x, mid))

        pl.when(inner)(jobs)

    def back(g):
        end = step_on(-1)

        def jobs():
            wait_block(g, recv.at[g.number, FROM_MID])
            added(g, [(terms(g, end) + [g.at(g.came, FROM_MID - FROM_END)], g.at(g.sums, end))],
                  lambda x: send_sum(g, end, LATE, FROM_END, end))

        pl.when(inner)(jobs)

    def last(gs):
        def places(k):
            g = gs[k]
            pool, first = (p3, k % 2) if g.rows > LANES else ((p1, p2)[k // 2 % 2], k % 2)
            return [pool.at[pl.ds((first * LINE + i) * g.rows, g.rows), pl.ds(0, g.columns)] for i in range(LINE)]

        def copies(k):
            g = gs[k]
            parts = terms(g, z) + [g.at(g.came, FROM_MID + 1 - FROM_END), g.at(g.came, jnp.where(at_end, 0, 2))]
            return [pltpu.make_async_copy(src, dst, load.at[k % AT_ONCE * LINE + i, 0]) for i, (src, dst) in enumerate(zip(parts, places(k)))]

        def out(k):
            return pltpu.make_async_copy(places(k)[0], gs[k].out, load.at[k % AT_ONCE, 1])

        def start(k):
            came = recv.at[gs[k].number]
            own, swapped, mid, end = copies(k)

            @pl.when(inner)
            def _():
                wait_block(gs[k], came.at[FROM_END + 2], came.at[FROM_MID + 1])
                mid.start()

            pl.when(at_end)(lambda: wait_block(gs[k], came.at[FROM_END]))
            for c in (own, swapped, end):
                c.start()

        def finish(k):
            own, swapped, mid, end = copies(k)
            for c in (own, swapped, end):
                c.wait()
            pl.when(inner)(mid.wait)
            own, swapped, mid, end = places(k)
            across = pl.ds(0, gs[k].columns)

            @pl.loop(0, gs[k].rows // PACK)
            def _(i):
                here = pl.ds(pl.multiple_of(i * PACK, PACK), PACK)
                total = own[here, :].astype(F32) + swapped[here, :].astype(F32) + end[here, :].astype(F32)
                low = jnp.where(inner, total + mid[here, :].astype(F32), total).astype(BF16)
                own[here, :] = low
                wide = low.astype(F32)
                square_s[:, across] += wide * wide

            out(k).start()

        for k in range(-2, len(gs)):
            if k >= 2:
                out(k - 2).wait()
            if k + 2 < len(gs):
                start(k + 2)
            if k >= 0:
                finish(k)
        for k in range(max(len(gs) - 2, 0), len(gs)):
            out(k).wait()


    wqkv_s, wo_s = p1.at[:, pl.ds(0, three)], p1.at[:, pl.ds(three, d)]

    def transposed_dot(lhs, w, here):
        return _dot_turned(lhs[...], w[here, :])

    def hidden(first, many):
        def part(j, here):
            gate = _dot(b_s[...], p1[:, here])
            up = _dot(b_s[...], p2[:, here])
            by = transposed_dot(by_s, p3, here).astype(BF16).astype(F32)
            sig = jax.nn.sigmoid(gate)
            bu_s[:, here] = (by * (gate * sig)).astype(BF16)
            bg_s[:, here] = (by * up * (sig * (1 + gate * (1 - sig)))).astype(BF16)

        width = p1.shape[1]

        @pl.loop(first, min(first + many, width // TILE))
        def _(j):
            part(j, pl.ds(pl.multiple_of(j * TILE, TILE), TILE))

        if first + many > width // TILE and width % TILE:
            part(width // TILE, pl.ds(width // TILE * TILE, width % TILE))

    def project_back(w, src, dst):
        def part(j, here):
            dst[:, here] = transposed_dot(src, w, here).astype(BF16)

        _tiles(d, part)

    def by_b():
        def part(j, here):
            bb_s[:, here] = (transposed_dot(bg_s, p1, here) + transposed_dot(bu_s, p2, here)).astype(BF16)

        _tiles(d, part)


    def layer_steps(n):
        s = outs[n]
        grad = lambda kind: of[n, kind]

        def start():
            fetch("hid_t", s["hid_t"], p3)
            for name, dst in (("b", b_s), ("g", p1), ("u", p2), ("heads", qkv_s), ("lse", lse_s), ("hm", hm_s), ("att", o_s)):
                fetch(name, s[name], dst)

        def by_down():
            need("hid_t")
            _rows_out(p3, by_s, high_s, grad("d").whole, store, 0, ff, ff // 10)
            fetch("d", s["d"], p3)

        def start_last():
            fetch("d", s["d"], p3)
            all_sent()
            for key in list(saving):
                kept(*key)

        def turned_b():
            if n < top:
                need("b")
            _flip(b_s, t_s)

        def hidden_first():
            need("d")
            if n < top:
                need("g", "u", "hm", "att", "heads", "lse")
            hidden(0, 4)

        def by_part(kind, src):
            g = grad(kind)
            _columns_out(t_s, src.at[:, g.across], wide_s, g.whole, store)

        def hidden_last():
            hidden(10, 3)
            fetch("a", s["a"], a_s)

        def by_mid():
            fetch("o", s["o"], wo_s)
            fetch("qkv", s["qkv"], wqkv_s)
            _norm_back(hm_s, bb_s, by_s)
            if n:
                fetch("h", outs[n - 1]["states"], hm_s)

        def by_o():
            _flip(o_s, t_s)
            _columns_out(t_s, by_s, wide_s, grad("o").whole, store)

        def by_att():
            need("o")
            project_back(wo_s, by_s, bb_s)

        def attention(iq):
            if iq == 0:
                dk_s[...] = jnp.zeros(dk_s.shape, F32)
                dv_s[...] = jnp.zeros(dv_s.shape, F32)
            _attend_rows_back(iq, qkv_s, o_s, bb_s, lse_s, bq_s, dq_s, dk_s, dv_s, cos_ref, sin_ref, HEAD**-0.5)

        def by_qkv():
            need("a", "qkv")
            _flip(a_s, t_s)
            _columns_out(t_s, bq_s, wide_s, grad("qkv").whole, store)

        def by_states():
            project_back(wqkv_s, bq_s, bb_s)
            need("h")
            _norm_back(hm_s, bb_s, by_s)

        f = functools.partial
        do = lambda what, *kinds: [f(what, grad(kind)) for kind in kinds]
        part = lambda kind: [f(by_part, kind, bg_s if kind[0] == "g" else bu_s)] + do(pair, kind)
        if n == top:
            steps = [start_last, turned_b, f(summed, grad("d"), "rest")] + do(late, "d") + [hidden_first]
        else:
            steps = [start, by_down] + do(pair, "d") + [f(passed, of[n + 1, "qkv"]), turned_b, hidden_first] + do(summed, "d") + [f(back, of[n + 1, "o"])]
        steps += [f(hidden, 4, 3)] + part("g0") + part("u0") + do(summed, "g0") + [f(hidden, 7, 3)] + do(summed, "u0") + [hidden_last]
        steps += do(passed, "d") + part("g1") + part("u1") + do(summed, "g1") + [by_b] + do(passed, "g0") + do(summed, "u1") + do(back, "d")
        steps += [by_mid, by_o] + do(pair, "o") + do(passed, "u0") + [by_att] + do(summed, "o") + do(back, "g0") + do(passed, "g1")
        steps += (do(late, "g0", "u0") if n == top else []) + do(back, "u0") + do(passed, "u1") + [f(attention, 0)] + do(back, "g1") + do(passed, "o")
        steps += (do(late, "g1", "u1") if n == top else []) + [f(attention, 1)] + do(back, "u1") + [by_qkv] + do(pair, "qkv")
        return steps + ([by_states] if n else []) + do(summed, "qkv") + (do(late, "o") if n == top else [])


    work = []
    f = functools.partial
    first = of[top, "d"]
    for n in range(layers):
        work += [((), 1.4, f(prepare, n)), ([(n, "qkv0"), (n, "qkv1")], 4, f(project, n, 0, 3)), ((), 2.4, f(project, n, 3, 3))]
        work.append(((), 4, f(attention_rows, n, 0, 1)))
        for iq in range(1, tokens // BQ):
            work += [((), 4, f(attention_rows, n, iq, 0)), ((), 4, f(attention_rows, n, iq, 1))]
        work += [([(n, "o")], 3, f(attended, n)), ((), 1.4, f(prepared, n))]
        for part in range(PARTS):
            tiles = held[f"g{part}"].shape[1] // LANES
            low = tiles // 2
            needs = [(n, f"g{part}"), (n, f"u{part}")]
            work += [(needs, low * 0.75 + 1, f(gated, n, part, 0, low)), ((), tiles * 0.75 / 2, f(gated, n, part, low, tiles - low))]
            if n == top:
                work.append(((), tiles * 0.35, f(last_down, part)))
                if part == PARTS - 2:
                    work.append(((), 0.1, f(pair, first, ENDS)))
            else:
                work.append(((), tiles * 0.25, f(flipped, n, part)))
        if n < top:
            work += [([(n, f"d{part}")], 4.5, f(down, n, part * d // 512, d // 512)) for part in range(2)]
    work.insert(-2, ((), 3, f(summed, first, "first")))
    work.append(((), 0, f(pair, first, INNERS)))
    square_s[...] = jnp.zeros(square_s.shape, F32)
    for stage, what in _schedule(units, work):
        what() if stage == "run" else arrived(stage, what)
    steps = layer_steps(top)
    for n in reversed(range(top)):
        steps += layer_steps(n)
    for step in steps:
        step()
    end = grads[-1]
    waiting = [of[0, kind] for kind in GRADS[:5]] + [of[top, "qkv"], of[0, "o"], end]
    sent_far(of[0, "u1"])
    for g in waiting[:2]:
        late(g)
    back(of[top, "qkv"])
    passed(end)
    back(of[0, "o"])
    last([of[top, kind] for kind in GRADS[:6]])
    back(end)
    sent_far(end)

    for g, following in zip(waiting, waiting[2:]):
        pl.when(at_end)(lambda g=g: wait_block(g, send.at[g.number, LATE]))
        late(following)
    last(waiting)

    table_s[way] = jnp.full(table_s.shape[1:], jnp.sum(square_s[...]), F32)
    copies = []
    for j, device in enumerate(peers):
        copies.append(pltpu.make_async_remote_copy(src_ref=table_s.at[way], dst_ref=table_s.at[way], send_sem=meet.at[0, j],
                                                   recv_sem=meet.at[1, j], device_id=device, device_id_type=MESH))
        copies[-1].start()
    for copy in copies:
        copy.wait()
    total = table_s[0]
    for j in range(1, WAYS):
        total = total + table_s[j]
    squares[...] = total

    for g in grads:
        for sent in (PAIR, PAIR_LAST):
            wait(g.at(g.swapped, 0, 2), send.at[g.number, sent])
        sent_late = lambda g=g: wait_block(g, send.at[g.number, LATE])
        pl.when(inner)(sent_late) if g in waiting[:-2] else sent_late()
        far = lambda g=g: wait_block(g, send.at[g.number, FAR_ONE], send.at[g.number, FAR_TWO])
        pl.when(inner)(far) if g in (end, of[0, "u1"]) else far()


def turning(tokens):
    side = math.isqrt(tokens)
    turn = float(THETA) ** (-np.arange(HEAD // 2) / (HEAD // 2))
    tables = []
    for places in (np.arange(side), np.arange(tokens // side) * side):
        cos, sin = (np.concatenate([f(places[:, None] * turn)] * 2, 1) for f in (np.cos, np.sin))
        tables += [cos, sin, np.where(np.arange(HEAD) < HEAD // 2, -sin, sin)]
    return np.stack(tables).astype(np.float32)


def both_passes(x, dy, weights):
    wq, wk, wv, wo, wg, wu, wd = weights
    layers, (tokens, wide) = wq.shape[0], x.shape
    ff, kv, heads = wg.shape[2], wk.shape[2], wide // HEAD
    three = wide + 2 * kv
    big = lambda *shape: jax.ShapeDtypeStruct(shape, BF16)
    whole = dict(qkv=big(wide, three), o=big(wide, wide), g=big(wide, ff), u=big(wide, ff), d=big(ff, wide))
    square = big(tokens, wide)
    saved = dict(a=square, heads=big(tokens, three), att=square, lse=jax.ShapeDtypeStruct((heads, tokens), F32), hm=square, b=square,
                 states=square, hid_t=big(ff, tokens))
    outs = [*whole.values(), *(saved[name] for name in SAVED)] * layers
    where = {}
    for n in reversed(range(layers)):
        for kind in GRAD_ARRAYS:
            rows, columns = whole[kind].shape
            part = rows // WAYS
            outs += [whole[kind], *[big(rows // 2, columns)] * 2, big(part * (CAME - FROM_END), columns), big(part, columns)]
            where[n, kind] = len(outs) - 1
    vm = lambda *shape: pltpu.VMEM(shape, BF16)
    f32 = lambda *shape: pltpu.VMEM(shape, F32)
    sems = lambda *shape: pltpu.SemaphoreType.DMA(shape)
    units, count = layers * len(KINDS), layers * len(GRADS)
    got = pl.pallas_call(
        functools.partial(_both_passes, layers),
        in_specs=[EVERY] * 9 + [INNER],
        out_specs=[EVERY] * len(outs) + [INNER],
        out_shape=[*outs, jax.ShapeDtypeStruct((8, LANES), F32)],
        scratch_shapes=[vm(wide, ff), vm(wide, ff), vm(ff, wide), vm(tokens, ff), vm(tokens, ff), *[vm(tokens, wide)] * 6, vm(tokens, three),
                        vm(tokens, three), f32(heads, HEAD + 8, BQ), *[f32(kv // HEAD, tokens, HEAD)] * 2, f32(heads, BQ), f32(heads, tokens),
                        vm(2, wide, TILE), vm(2, (ff - 2 * (-(-ff // LINE // LANES) * LANES)) // 4, wide), f32(PACK, p_half(ff)), f32(WAYS, 8, LANES), f32(tokens, HEAD), f32(tokens, HEAD),
                        sems(units, OWN + 1), sems(units, OWN + 1), sems(units, 2), sems(layers, len(WHOLE)), sems(layers, len(SAVED)),
                        sems(count, PAIR_LAST + 1), sems(count, CAME + 1), sems(len(FETCHED)), sems(2), sems(2, WAYS - 1)],
        compiler_params=pltpu.CompilerParams(collective_id=0, has_side_effects=True, vmem_limit_bytes=67043328),
        cost_estimate=pl.CostEstimate(flops=270 * 10**9, bytes_accessed=6 * 10**8, transcendentals=10**7),
        name="both_passes",
    )(x, dy, *weights, turning(tokens))
    return [{kind: got[where[n, kind]] for kind in GRAD_ARRAYS} for n in range(layers)], got[-1]


def _step(layers, count, squares, *refs):
    kinds = len(NAMES)
    w, m, v = refs[:kinds], refs[kinds : 2 * kinds], refs[2 * kinds : 3 * kinds]
    refs = refs[3 * kinds :]
    grads, refs = [dict(zip(GRAD_ARRAYS, refs[n * len(GRAD_ARRAYS) :])) for n in range(layers)], refs[layers * len(GRAD_ARRAYS) :]
    outs, refs = refs[: 3 * kinds], refs[3 * kinds :]
    held, g_held, came, g_came, left = refs[: 3 * kinds], dict(zip(GRAD_ARRAYS, refs[3 * kinds :])), *refs[-3:]
    of = dict(zip(NAMES, [("qkv", 0), ("qkv", w[0].shape[2]), ("qkv", w[0].shape[2] + w[1].shape[2]), ("o", 0), ("g", 0), ("u", 0), ("d", 0)]))
    reads = {}
    for n in range(layers):
        for i, kind in enumerate(GRAD_ARRAYS):
            reads[n, kind] = pltpu.make_async_copy(grads[n][kind], g_held[kind].at[n], g_came.at[n, i])
            reads[n, kind].start()
        for i in range(kinds):
            for x, src in enumerate((w[i], m[i], v[i])):
                reads[n, i, x] = pltpu.make_async_copy(src.at[n], held[x * kinds + i].at[n], came.at[n, i, x])
                reads[n, i, x].start()
    factor = jnp.minimum(1.0, 0.5 * lax.rsqrt(squares[...] / count + 1e-30))[:1, :1]
    writes = []
    for n in range(layers):
        for i, name in enumerate(NAMES):
            kind, first = of[name]
            if (n, kind) in reads:
                reads.pop((n, kind)).wait()
            for x in range(3):
                reads[n, i, x].wait()
            w_s, m_s, v_s = (held[x * kinds + i].at[n] for x in range(3))
            g_s = g_held[kind].at[n, :, pl.ds(first, w_s.shape[1])]

            @pl.loop(0, w_s.shape[0] // PACK)
            def _(j):
                rows = pl.ds(pl.multiple_of(j * PACK, PACK), PACK)
                g, old = g_s[rows, :].astype(F32) * factor, w_s[rows, :].astype(F32)
                new_m = 0.9 * m_s[rows, :] + 0.1 * g
                new_v = 0.95 * v_s[rows, :] + 0.05 * g * g
                m_s[rows, :] = new_m
                v_s[rows, :] = new_v
                w_s[rows, :] = (old - 0.02 * (new_m * lax.rsqrt(new_v + 1e-8) + 0.1 * old)).astype(BF16)

            for x, src in enumerate((w_s, m_s, v_s)):
                writes.append(pltpu.make_async_copy(src, outs[x * kinds + i].at[n], left.at[n, i, x]))
                writes[-1].start()
    for copy in writes:
        copy.wait()


def take_step(squares, weights, m, v, parts):
    layers, kinds = weights[0].shape[0], len(weights)
    sems = lambda *shape: pltpu.SemaphoreType.DMA(shape)
    like = [jax.ShapeDtypeStruct(t.shape, t.dtype) for t in (*weights, *m, *v)]
    return pl.pallas_call(
        functools.partial(_step, layers, WAYS * sum(t.size for t in weights)),
        in_specs=[INNER] + [EVERY] * (3 * kinds + layers * len(GRAD_ARRAYS)),
        out_specs=[EVERY] * len(like),
        out_shape=like,
        scratch_shapes=[pltpu.VMEM(t.shape, t.dtype) for t in like] + [pltpu.VMEM((layers, *parts[0][kind].shape), BF16) for kind in GRAD_ARRAYS]
        + [sems(layers, kinds, 3), sems(layers, len(GRAD_ARRAYS)), sems(layers, kinds, 3)],
        compiler_params=pltpu.CompilerParams(vmem_limit_bytes=67043328),
        name="take_step",
    )(squares, *weights, *m, *v, *[part[kind] for part in parts for kind in GRAD_ARRAYS])


def solution(mesh):
    def step(x, dy, *arrays):
        weights, m, v = (arrays[i : i + len(NAMES)] for i in range(0, len(arrays), len(NAMES)))
        parts, squares = both_passes(x[0], dy[0], weights)
        return tuple(take_step(squares, weights, m, v, parts))

    states, cut = P(("rep", "dp"), None, None), P(None, "dp", None)
    return jax.shard_map(
        step,
        mesh=mesh,
        in_specs=(states, states) + (cut,) * 21,
        out_specs=(P("rep", "dp", None),) * 21,
        check_vma=False,
    )
```
